256 devices in a mesh: seq: 16 (over z, core), grp: 2 (over y_hi), dp: 8 (over y_lo, x).
Axes of the slice: x: 4, y: 4 (y_hi: 2, y_lo: 2; y = y_hi * 2 + y_lo), z: 8, core: 2. Of those that a mesh axis runs over, the one named last changes fastest.
Arguments:
- clips: bfloat16 [8, 2048, 1408], P('dp', 'seq'), may hold values from -6 to 6
- context: int32 [8, 2048], P('dp', 'seq'), may hold values from 0 to 1, as said below
- predict_index: int32 [8, 3072], P('dp', 'seq'), may hold values from -1 to 2047, as said below
- target_qkv: bfloat16 [3, 1408, 1408], P(None, 'dp', 'grp'), may hold values from -8 to 8
- target_out: bfloat16 [1408, 1408], P('grp'), may hold values from -0.15625 to 0.15625
- student_qkv: bfloat16 [3, 1408, 1408], P(None, 'dp', 'grp'), may hold values from -8 to 8
- student_out: bfloat16 [1408, 1408], P('grp', 'dp'), may hold values from -0.15625 to 0.15625
- mask_token: float32 [1408], replicated, may hold values from -4 to 4
Outputs:
- out_grad: float32 [1408, 1408], P('grp', 'dp')
- target_blend: float32 [1408, 1408], P('grp')
The draws below stay inside these ranges and needn't reach their ends.
Inputs may be any that keep to these rules, and one draw needn't show every extreme that they name: In every aligned block of 128 tokens of a clip exactly 32 tokens have context 1 and the others 0. `predict_index`: each device's 192 slots name distinct target positions (context 0) of its clip, followed by -1 in the unused slots; different devices' lists may name the same position. In every clip one list is full.
All inputs are finite; a program needn't handle non-finite values.
Results may differ from the reference program's by a relative error of at most 0.014.
Values may be sent and summed in bfloat16 or wider, within the bound.
No kernel may reach another device: no remote copies, remote signals or barrier semaphores. Data moves between devices by JAX's collectives and lax.ppermute only.
A program may use at most 128 MiB of HBM per device.

```python
import math
import jax
import jax.numpy as jnp
from jax import lax

D = 1408
HEAD_DIM = 88
TOK_DEV = 128
TGT_DEV = 96
SLOTS = 192
TOKENS = 2048
CLIPS = 8
N_GRP = 2


def draw_plan(base_key):
    shard_total = TOKENS // TOK_DEV
    stream = jax.random.fold_in(base_key, 11)
    clip_keys = jax.random.split(stream, CLIPS)

    def one_clip(clip_key):
        mask_key, pick_key, load_key, busy_key = jax.random.split(clip_key, 4)
        shard_keys = jax.random.split(mask_key, shard_total)
        shuffled = jax.vmap(lambda single: jax.random.permutation(single, TOK_DEV))(shard_keys)
        is_target = (shuffled < TGT_DEV).reshape(TOKENS)
        flags = jnp.where(is_target, 0, 1).astype(jnp.int32)
        busiest = jax.random.randint(busy_key, (), 0, shard_total)
        loads = jax.random.randint(load_key, (shard_total,), TGT_DEV // 2, TGT_DEV + 1)
        devices = jnp.arange(shard_total, dtype=jnp.int32)
        counts = jnp.where(devices == busiest, SLOTS, loads).astype(jnp.int32)
        pick_keys = jax.random.split(pick_key, shard_total)

        def one_list(single, count):
            ordering = jax.random.permutation(single, TOKENS).astype(jnp.int32)
            ranking = jnp.where(is_target, ordering, TOKENS + ordering)
            chosen = jnp.argsort(ranking, stable=True)[:SLOTS].astype(jnp.int32)
            slot_ids = jnp.arange(SLOTS, dtype=jnp.int32)
            return jnp.where(slot_ids < count, chosen, -1).astype(jnp.int32)
        lists = jax.vmap(one_list)(pick_keys, counts)
        return (flags, lists.reshape(shard_total * SLOTS))
    return jax.vmap(one_clip)(clip_keys)


def mask_vector(base_key):
    return jnp.clip(jax.random.normal(jax.random.fold_in(base_key, 31), (D,), jnp.float32), -4.0, 4.0)


def draw_weights(base_key, salt):
    local_key = jax.random.fold_in(base_key, salt)
    base_key_two = jax.random.fold_in(local_key, 0)
    scale = D ** (-0.5)
    base = jnp.clip(jax.random.normal(base_key_two, (3, D, D), jnp.float32), -6.0, 6.0) * scale
    return base


def draw_target_qkv(key, part):
    return draw_weights(key, 41).astype(jnp.bfloat16)


def draw_student_qkv(key, part):
    return draw_weights(key, 43).astype(jnp.bfloat16)


def draw_mask_token(key, part):
    return mask_vector(key)


def draw_clips(key, part):
    noise_key = jax.random.fold_in(key, 37)
    first_key = jax.random.fold_in(noise_key, 0)
    base = jnp.clip(jax.random.normal(first_key, (CLIPS, TOKENS, D), jnp.float32), -5.0, 5.0)
    return base.astype(jnp.bfloat16)


def draw_context(key, part):
    return draw_plan(key)[0]


def draw_predict_index(key, part):
    return draw_plan(key)[1]


def block_levels(stream_key, dims, cuts, smallest, largest):
    def one(dim, blocks):
        draws = jax.random.uniform(jax.random.fold_in(jax.random.fold_in(stream_key, 6), dim), (blocks,), jnp.float32, smallest / len(cuts), largest / len(cuts))
        return jnp.repeat(jnp.exp(draws), dims[dim] // blocks).reshape((-1,) + (1,) * (len(dims) - dim - 1))

    loudness = one(*cuts[0])
    for cut in cuts[1:]:
        loudness = loudness * one(*cut)
    return loudness


def scatter_about(stream_key, extent, scale, bound, pieces=(), kind=jnp.bfloat16):
    drawn = scale * jax.random.normal(stream_key, extent, jnp.float32)
    if pieces:
        drawn = drawn * block_levels(stream_key, extent, pieces, -0.22, 0.18)
    return jnp.clip(drawn, -bound, bound).astype(kind)


def setup_inputs(seed: int = 0) -> dict:
    keys = jax.random.split(jax.random.key(seed), 9)
    clips = draw_clips(jax.random.fold_in(keys[8], 71), 0)
    context = draw_context(jax.random.fold_in(keys[8], 71), 0)
    predict_index = draw_predict_index(jax.random.fold_in(keys[8], 71), 0)
    target_qkv = draw_target_qkv(jax.random.fold_in(keys[8], 71), 0)
    target_out = scatter_about(keys[4], (D, D), D ** -0.5, 0.15625, ((0, 2),))
    student_qkv = draw_student_qkv(jax.random.fold_in(keys[8], 71), 0)
    student_out = scatter_about(keys[6], (D, D), D ** -0.5, 0.15625, ((0, 2), (1, 8)))
    mask_token = draw_mask_token(jax.random.fold_in(keys[8], 71), 0)
    return dict(clips=clips, context=context, predict_index=predict_index, target_qkv=target_qkv, target_out=target_out, student_qkv=student_qkv, student_out=student_out, mask_token=mask_token)


EPSILON = 1e-06
MOMENTUM = 0.99

def layer_norm(values):
    center = values - lax.optimization_barrier(jnp.mean(values, axis=-1, keepdims=True))
    factor = lax.rsqrt(lax.optimization_barrier(jnp.mean(center * center, axis=-1, keepdims=True)) + EPSILON)
    return (center * factor, factor)

def position_table(places, width):
    half_width = width // 2
    spacing = jnp.exp(jnp.arange(half_width, dtype=jnp.float32) * (-math.log(10000.0) / half_width))
    angles = places.astype(jnp.float32)[:, None] * spacing[None, :]
    return jnp.concatenate([jnp.sin(angles), jnp.cos(angles)], axis=1)

def attention(queries, key_rows, value_rows, allowed):
    width = queries.shape[1]
    head_count = width // HEAD_DIM
    query_heads = queries.reshape(queries.shape[0], head_count, HEAD_DIM).transpose(1, 0, 2)
    key_heads = key_rows.reshape(key_rows.shape[0], head_count, HEAD_DIM).transpose(1, 0, 2)
    value_heads = value_rows.reshape(value_rows.shape[0], head_count, HEAD_DIM).transpose(1, 0, 2)
    factor = HEAD_DIM ** (-0.5)

    def one_head(triple):
        query_block, key_block, value_block = triple
        scores = jnp.dot(query_block, key_block.T, preferred_element_type=jnp.float32) * factor
        scores = jnp.where(allowed[None, :], scores, -jnp.inf)
        shifted = jnp.exp(scores - lax.optimization_barrier(jnp.max(scores, axis=1, keepdims=True)))
        mixed = jnp.dot(shifted.astype(jnp.bfloat16), value_block, preferred_element_type=jnp.float32)
        return mixed / lax.optimization_barrier(jnp.sum(shifted, axis=1, keepdims=True))
    outputs = lax.map(one_head, (query_heads, key_heads, value_heads))
    return outputs.transpose(1, 0, 2).reshape(queries.shape[0], width).astype(jnp.bfloat16)

def split_project(mixed, weight):
    part_width = mixed.shape[1] // N_GRP
    result = jnp.zeros((mixed.shape[0], weight.shape[1]), jnp.float32)
    for member in range(N_GRP):
        partial_sum = jnp.dot(mixed[:, member * part_width:(member + 1) * part_width], weight[member * part_width:(member + 1) * part_width], preferred_element_type=jnp.float32)
        result = result + lax.optimization_barrier(partial_sum.astype(jnp.bfloat16)).astype(jnp.float32)
    return result

def clip_gradient(tokens, context, listed, target_qkv, target_out, student_qkv, student_out, mask_token):
    width = tokens.shape[1]
    normed = layer_norm(tokens.astype(jnp.float32))[0].astype(jnp.bfloat16)
    query_t = jnp.dot(normed, target_qkv[0], preferred_element_type=jnp.float32).astype(jnp.bfloat16)
    key_t = jnp.dot(normed, target_qkv[1], preferred_element_type=jnp.float32).astype(jnp.bfloat16)
    value_t = jnp.dot(normed, target_qkv[2], preferred_element_type=jnp.float32).astype(jnp.bfloat16)
    everyone = jnp.ones((tokens.shape[0],), dtype=bool)
    target_mixed = attention(query_t, key_t, value_t, everyone)
    target_sum = split_project(target_mixed, target_out)
    target_features = layer_norm(tokens.astype(jnp.float32) + target_sum)[0].astype(jnp.bfloat16)
    context_keys = jnp.dot(normed, student_qkv[1], preferred_element_type=jnp.float32).astype(jnp.bfloat16)
    context_values = jnp.dot(normed, student_qkv[2], preferred_element_type=jnp.float32).astype(jnp.bfloat16)
    seeds = mask_token[None, :] + position_table(jnp.arange(tokens.shape[0], dtype=jnp.int32), width)
    seed_normed = layer_norm(seeds)[0].astype(jnp.bfloat16)
    seed_queries = jnp.dot(seed_normed, student_qkv[0], preferred_element_type=jnp.float32).astype(jnp.bfloat16)
    student_mixed = attention(seed_queries, context_keys, context_values, context == 1)
    student_sum = split_project(student_mixed, student_out)
    predicted, factor = layer_norm(seeds + student_sum)
    usable = (listed >= 0).astype(jnp.float32)
    counts = jnp.zeros((tokens.shape[0],), jnp.float32).at[jnp.maximum(listed, 0).astype(jnp.int32)].add(usable)
    slope = jnp.clip(predicted - target_features.astype(jnp.float32), -1.0, 1.0) * counts[:, None]
    back_grad = (slope - lax.optimization_barrier(jnp.mean(slope, axis=1, keepdims=True)) - predicted * lax.optimization_barrier(jnp.mean(slope * predicted, axis=1, keepdims=True))) * factor
    return jnp.dot(student_mixed.astype(jnp.float32).T, back_grad, precision=lax.Precision.HIGHEST)

def reference(clips, context, predict_index, target_qkv, target_out, student_qkv, student_out, mask_token):

    def advance(running, inputs):
        tokens, flags, listed = inputs
        return (running + clip_gradient(tokens, flags, listed, target_qkv, target_out, student_qkv, student_out, mask_token), None)
    out_grad, unused = lax.scan(advance, jnp.zeros((D, D), jnp.float32), (clips, context, predict_index))
    target_blend = MOMENTUM * target_out.astype(jnp.float32) + (1.0 - MOMENTUM) * student_out.astype(jnp.float32)
    return (out_grad, target_blend)
```

```python
import math

import jax
import jax.numpy as jnp
from jax import lax
from jax.sharding import Mesh, PartitionSpec as P

HEAD_DIM = 88
PART = 44
PAD = 64
LANES = 128
CTX = 32
BLOCK = 128
TGT = 96
OWN = 48
EPSILON = 1e-06
MOMENTUM = 0.99
BF = jnp.bfloat16
F32 = jnp.float32
SWAP = [(0, 1), (1, 0)]
DP = ("ylo", "x")


def to_all(shard, axes, count):
    copies = jnp.broadcast_to(shard[None], (count, *shard.shape))
    return lax.all_to_all(copies, axes, split_axis=0, concat_axis=0, tiled=True)


def layer_norm(values):
    center = values - jnp.mean(values, axis=-1, keepdims=True)
    factor = lax.rsqrt(jnp.mean(center * center, axis=-1, keepdims=True) + EPSILON)
    return (center * factor, factor)


def spacing_of(half):
    return jnp.exp(jnp.arange(half, dtype=F32) * (-math.log(10000.0) / half))


def mm(a, b):
    return jnp.dot(a, b, preferred_element_type=F32)


def attention(queries, keys, values):
    scores = lax.dot_general(
        queries, keys, (((1,), (1,)), ((), ())), preferred_element_type=F32
    ) * (HEAD_DIM ** (-0.5))
    shifted = jnp.exp(scores - jnp.max(scores, axis=1, keepdims=True))
    mixed = mm(shifted.astype(BF), values)
    return (mixed / jnp.sum(shifted, axis=1, keepdims=True)).astype(BF)


def ring(rows, n):
    chunk = rows.shape[0] // 2
    up = [(i, (i + 1) % n) for i in range(n)]
    down = [(i, (i - 1) % n) for i in range(n)]
    pieces = [rows[:chunk], rows[chunk:]]
    slots = {0: list(pieces)}
    for d in range(1, n):
        slots[d] = [None, None]
    ups, downs = list(pieces), list(pieces)
    for step in range(1, n // 2 + 1):
        for c in range(2):
            if step < n // 2 or c == 0:
                ups[c] = lax.ppermute(ups[c], "z", up)
                slots[step][c] = ups[c]
            if step < n // 2 or c == 1:
                downs[c] = lax.ppermute(downs[c], "z", down)
                slots[n - step][c] = downs[c]
    return slots


def body(
    clips, context, predict_index, target_qkv, target_out, student_qkv, student_out, mask_token
):
    tokens = clips[0]
    width = tokens.shape[1]
    half = width // 2
    n_z = lax.axis_size("z")
    n_dp = lax.axis_size("ylo") * lax.axis_size("x")
    z = lax.axis_index("z")
    core = lax.axis_index("core")
    grp = lax.axis_index("grp")
    heads = target_qkv.shape[2] // HEAD_DIM

    col = jnp.arange(target_qkv.shape[2], dtype=jnp.int32)[:, None]
    lane = jnp.arange(LANES, dtype=jnp.int32)[None, :]
    plain = ((col == z * HEAD_DIM + lane) & (lane < HEAD_DIM)).astype(BF)
    in_half = lane % PAD
    halved = (
        (col == z * HEAD_DIM + (lane // PAD) * PART + in_half) & (in_half < PART)
    ).astype(BF)
    chosen = jnp.where(core == 0, target_qkv, student_qkv)
    head_qk = jnp.einsum("krc,cn->krn", chosen[:2], plain, preferred_element_type=F32)
    head_v = jnp.einsum("krc,cn->krn", chosen[2:], halved, preferred_element_type=F32)
    head_mine = jnp.concatenate([head_qk, head_v], axis=0).astype(BF)
    weight_mine = to_all(head_mine, DP, n_dp)
    weight_mine = jnp.moveaxis(weight_mine, 0, 1).reshape(3, width, LANES)
    weight_other = lax.ppermute(weight_mine, "core", SWAP)
    weight_t = jnp.where(core == 0, weight_mine, weight_other)
    weight_s = jnp.where(core == 0, weight_other, weight_mine)

    flag = (context[0] == 1).astype(jnp.int32)
    t_row = jnp.arange(BLOCK, dtype=jnp.int32)
    upto = t_row[:, None] <= t_row[None, :]
    before = jnp.sum(jnp.where(upto, flag[:, None], 0), axis=0)
    rank = jnp.where(flag == 1, before - 1, CTX + t_row - before)
    perm = (rank[None, :] == t_row[:, None]).astype(BF)
    normed = layer_norm(tokens.astype(F32))[0].astype(BF)
    normed_p = mm(perm, normed).astype(BF)
    slots = ring(normed_p, n_z)

    spacing = spacing_of(half)
    t_angle = t_row.astype(F32)[:, None] * spacing[None, :]
    t_sin, t_cos = (jnp.sin(t_angle), jnp.cos(t_angle))
    base = ((2 * jnp.arange(n_z, dtype=jnp.int32) + core) * BLOCK).astype(F32)
    b_angle = base[:, None] * spacing[None, :]
    b_sin, b_cos = (jnp.sin(b_angle)[:, None], jnp.cos(b_angle)[:, None])
    seed_a = b_sin * t_cos[None] + b_cos * t_sin[None] + mask_token[None, None, :half]
    seed_b = b_cos * t_cos[None] - b_sin * t_sin[None] + mask_token[None, None, half:]
    mean = (jnp.sum(seed_a, -1, keepdims=True) + jnp.sum(seed_b, -1, keepdims=True)) / width
    seed_a, seed_b = (seed_a - mean, seed_b - mean)
    var = (
        jnp.sum(seed_a * seed_a, -1, keepdims=True) + jnp.sum(seed_b * seed_b, -1, keepdims=True)
    ) / width
    inv = lax.rsqrt(var + EPSILON)
    seed_a = (seed_a * inv).astype(BF).reshape(n_z * BLOCK, half)
    seed_b = (seed_b * inv).astype(BF).reshape(n_z * BLOCK, half)
    query_s = (mm(seed_a, weight_s[0, :half]) + mm(seed_b, weight_s[0, half:])).astype(BF)

    listed = predict_index[0]
    listed = jnp.concatenate([listed, lax.ppermute(listed, "core", SWAP)])
    places = (
        (2 * jnp.arange(n_z, dtype=jnp.int32)[:, None] + core) * BLOCK + t_row[None, :]
    ).reshape(-1)
    count_part = jnp.sum((places[:, None] == listed[None, :]).astype(F32), axis=1)

    half_rows = student_out.shape[0] // 2
    so_mine = lax.dynamic_slice_in_dim(student_out, core * half_rows, half_rows, axis=0)
    so_mine = jnp.moveaxis(to_all(so_mine, DP, n_dp), 0, 1).reshape(half_rows, width)
    so_other = lax.ppermute(so_mine, "core", SWAP)
    relaid = jnp.where(
        core == 0,
        jnp.concatenate([so_mine, so_other], axis=0),
        jnp.concatenate([so_other, so_mine], axis=0),
    )
    target_blend = MOMENTUM * target_out.astype(F32) + (1.0 - MOMENTUM) * relaid.astype(F32)

    def padded(rows):
        parts = rows.reshape(2 * heads, PART, width)
        parts = jnp.pad(parts, ((0, 0), (0, PAD - PART), (0, 0)))
        return parts.reshape(2 * heads * PAD, width)

    target_out_p = padded(target_out)
    student_out_p = padded(relaid)

    w_qkv = jnp.concatenate([weight_t[0], weight_t[1], weight_t[2]], axis=1)
    w_kv_s = jnp.concatenate([weight_s[1], weight_s[2]], axis=1)
    order = [0, 1, n_z - 1, 2, n_z - 2, 3, n_z - 3, 4]
    queries, kv_t, kv_s = ({}, [], [])
    for d in order:
        first, second = slots[d]
        one = mm(first, w_qkv).astype(BF)
        two = mm(second, w_qkv).astype(BF)
        queries[d] = jnp.concatenate([one[CTX:, :LANES], two[:, :LANES]], axis=0)
        kv_t += [one[:, LANES:], two[:, LANES:]]
        kv_s.append(mm(first[:CTX], w_kv_s).astype(BF))
    kv_s = jnp.concatenate(kv_s, axis=0)
    kv_s = jnp.concatenate([kv_s, lax.ppermute(kv_s, "core", SWAP)], axis=0)
    kv_t = jnp.concatenate(kv_t, axis=0)
    kv_t = jnp.concatenate([kv_t, lax.ppermute(kv_t, "core", SWAP)], axis=0)

    mixed_s = attention(query_s, kv_s[:, :LANES], kv_s[:, LANES:])
    mixed_s = jnp.where(lane == PART, count_part[:, None].astype(BF), mixed_s)
    mixed_s = lax.all_to_all(
        mixed_s.reshape(n_z, BLOCK, LANES), "z", split_axis=0, concat_axis=0, tiled=True
    )
    mixed_s = jnp.moveaxis(mixed_s, 0, 1).reshape(BLOCK, heads * LANES)
    mixed_sel = mm(perm[CTX:], mixed_s).astype(BF)
    usable = sum(mixed_sel[:, h * LANES + PART].astype(F32) for h in range(n_z))
    part_s = mm(mixed_sel, student_out_p).astype(BF).reshape(2, OWN, width)
    part_s_keep = jnp.where(grp == 0, part_s[0], part_s[1])
    part_s_send = jnp.where(grp == 0, part_s[1], part_s[0])
    sum_s = part_s_keep.astype(F32) + lax.ppermute(part_s_send, "grp", SWAP).astype(F32)
    mixed_all = to_all(mixed_sel, DP, n_dp).reshape(n_dp * TGT, heads * LANES)

    rows_own = lax.dynamic_slice_in_dim(perm, CTX + grp * OWN, OWN, axis=0)
    tokens_own = mm(rows_own, tokens)
    places_own = jnp.sum(rows_own.astype(F32) * t_row.astype(F32)[None, :], axis=1)
    places_own = places_own + ((2 * z + core) * BLOCK).astype(F32)
    angle = places_own[:, None] * spacing[None, :]
    seeds = mask_token[None, :] + jnp.concatenate([jnp.sin(angle), jnp.cos(angle)], axis=1)
    predicted, factor = layer_norm(seeds + sum_s)
    usable = lax.dynamic_slice_in_dim(usable, grp * OWN, OWN, axis=0)

    query_t = jnp.concatenate([queries[d] for d in range(n_z)], axis=0)
    mixed_t = attention(query_t, kv_t[:, :LANES], kv_t[:, LANES:]).reshape(n_z, TGT, LANES)
    flipped = jnp.concatenate([mixed_t[:1], mixed_t[:0:-1]], axis=0)
    twice = jnp.concatenate([flipped, flipped], axis=0)
    mixed_t = lax.dynamic_slice_in_dim(twice, (n_z - z) % n_z, n_z, axis=0)
    mixed_t = lax.all_to_all(mixed_t, "z", split_axis=0, concat_axis=0, tiled=True)
    mixed_t = jnp.moveaxis(mixed_t, 0, 1).reshape(TGT, heads * LANES)
    part_t = mm(mixed_t, target_out_p).astype(BF).reshape(2, OWN, width)
    part_t_keep = jnp.where(grp == 0, part_t[0], part_t[1])
    part_t_send = jnp.where(grp == 0, part_t[1], part_t[0])
    sum_t = part_t_keep.astype(F32) + lax.ppermute(part_t_send, "grp", SWAP).astype(F32)
    wanted = layer_norm(tokens_own + sum_t)[0].astype(BF).astype(F32)

    slope = jnp.clip(predicted - wanted, -1.0, 1.0) * usable[:, None]
    back_grad = (
        slope
        - jnp.mean(slope, axis=1, keepdims=True)
        - predicted * jnp.mean(slope * predicted, axis=1, keepdims=True)
    ) * factor
    columns = jnp.moveaxis(back_grad.astype(BF).reshape(OWN, n_dp, width // n_dp), 1, 0)
    arrived = lax.all_to_all(
        jnp.concatenate([columns, columns], axis=0),
        ("grp", *DP),
        split_axis=0,
        concat_axis=0,
        tiled=True,
    )
    arrived = jnp.moveaxis(arrived.reshape(2, n_dp, OWN, -1), 0, 1).reshape(n_dp * TGT, -1)
    grad = lax.dot_general(
        mixed_all, arrived, (((0,), (0,)), ((), ())), preferred_element_type=F32
    )
    grad = grad.reshape(heads, 2, PAD, -1)[:, :, :OWN]
    grad_keep = jnp.where(core == 0, grad[:, 0], grad[:, 1])
    grad_send = jnp.where(core == 0, grad[:, 1], grad[:, 0])
    grad = grad_keep + lax.ppermute(grad_send, "core", SWAP)
    grad = lax.all_to_all(grad.astype(BF), "z", split_axis=0, concat_axis=0, tiled=True)
    grad = jnp.sum(grad.astype(F32), axis=0)
    grad = to_all(grad.astype(BF), "z", n_z)
    other = lax.ppermute(grad, "core", SWAP)
    both = jnp.stack([jnp.where(core == 0, grad, other), jnp.where(core == 0, other, grad)], axis=1)
    out_grad = both[:, :, :PART].reshape(heads * HEAD_DIM, -1).astype(F32)
    return (out_grad, target_blend)


def solution(mesh):
    fine = Mesh(mesh.devices.reshape(8, 2, 2, 2, 4), ("z", "core", "grp", "ylo", "x"))
    seq = ("z", "core")
    in_specs = (
        P(DP, seq, None),
        P(DP, seq),
        P(DP, seq),
        P(None, DP, "grp"),
        P("grp", None),
        P(None, DP, "grp"),
        P("grp", DP),
        P(),
    )
    out_specs = (P("grp", DP), P("grp", None))
    return jax.shard_map(body, mesh=fine, in_specs=in_specs, out_specs=out_specs, check_vma=False)
```

```python
import functools
import math

import jax
import jax.numpy as jnp
from jax import lax
from jax.experimental import pallas as pl
from jax.experimental.pallas import tpu as pltpu
from jax.sharding import Mesh, PartitionSpec as P

HEAD_DIM = 88
LANES = 128
CTX = 32
BLOCK = 128
TGT = 96
OWN = 48
N_Z = 8
N_DP = 8
STRIPE = 11
EPSILON = 1e-06
MOMENTUM = 0.99
SCALE = HEAD_DIM ** (-0.5)
BF = jnp.bfloat16
F32 = jnp.float32
I32 = jnp.int32
SWAP = [(0, 1), (1, 0)]
DP = ("ylo", "x")
SMEM = pl.BlockSpec(memory_space=pltpu.SMEM)


def iota(shape, dim):
    return lax.broadcasted_iota(I32, shape, dim)


def mm(a, b):
    return jnp.dot(a, b, preferred_element_type=F32)


def mm_nt(a, b):
    return lax.dot_general(a, b, (((1,), (1,)), ((), ())), preferred_element_type=F32)


def sds(shape, dtype):
    return jax.ShapeDtypeStruct(shape, dtype)


def call(kernel, outs, scratch=(), flops=10**8, name=None, **specs):
    return pl.pallas_call(
        kernel,
        out_shape=outs,
        scratch_shapes=list(scratch),
        **specs,
        cost_estimate=pl.CostEstimate(flops=flops, bytes_accessed=10**6, transcendentals=0),
        name=name,
    )


def to_all(shard, axes, count):
    copies = jnp.broadcast_to(shard[None], (count, *shard.shape))
    return lax.all_to_all(copies, axes, split_axis=0, concat_axis=0, tiled=True)


def normalized(values):
    center = values - jnp.mean(values, axis=-1, keepdims=True)
    factor = lax.rsqrt(jnp.mean(center * center, axis=-1, keepdims=True) + EPSILON)
    return (center * factor, factor)


def sorted_norm_kernel(tokens_ref, context_ref, first_ref, second_ref, perm_ref):
    normed = normalized(tokens_ref[...].astype(F32))[0].astype(BF)
    flag = jnp.where(context_ref[...] == 1, 1.0, 0.0)
    upto = jnp.where(iota((BLOCK, BLOCK), 0) <= iota((BLOCK, BLOCK), 1), 1.0, 0.0).astype(BF)
    before = mm(jnp.broadcast_to(flag, (16, BLOCK)).astype(BF), upto)[:1]
    spot = iota((1, BLOCK), 1).astype(F32)
    rank = jnp.where(flag == 1.0, before - 1.0, CTX + spot - before).astype(I32)
    perm = jnp.where(rank == iota((BLOCK, BLOCK), 0), 1.0, 0.0).astype(BF)
    moved = mm(perm, normed).astype(BF)
    first_ref[...] = moved[: BLOCK // 2]
    second_ref[...] = moved[BLOCK // 2 :]
    perm_ref[...] = perm


def seed_query_kernel(sin_ref, cos_ref, bsin_ref, bcos_ref, mask_ref, weight_ref, out_ref):
    half = sin_ref.shape[1]

    def one(j, carry):
        bsin = bsin_ref[pl.ds(j, 1), :]
        bcos = bcos_ref[pl.ds(j, 1), :]
        t_sin = sin_ref[...]
        t_cos = cos_ref[...]
        a = bsin * t_cos + bcos * t_sin + mask_ref[0:1, :]
        b = bcos * t_cos - bsin * t_sin + mask_ref[1:2, :]
        mean = (jnp.sum(a, -1, keepdims=True) + jnp.sum(b, -1, keepdims=True)) / (2 * half)
        a = a - mean
        b = b - mean
        var = (jnp.sum(a * a, -1, keepdims=True) + jnp.sum(b * b, -1, keepdims=True)) / (2 * half)
        inv = lax.rsqrt(var + EPSILON)
        at = pl.multiple_of(j * BLOCK, BLOCK)
        query = mm((a * inv).astype(BF), weight_ref[:half, 3 * LANES : 4 * LANES])
        query = query + mm((b * inv).astype(BF), weight_ref[half:, 3 * LANES : 4 * LANES])
        out_ref[pl.ds(at, BLOCK), :] = query.astype(BF)
        return carry

    lax.fori_loop(0, N_Z, one, 0)


def project_kernel(z_ref, *refs):
    pieces = refs[: 2 * N_Z]
    weight_ref, query_ref, kv_ref, kvs_ref, rows_ref, ctx_ref = refs[2 * N_Z :]
    for d in range(N_Z):
        for c in range(2):
            at = d * BLOCK + c * BLOCK // 2
            rows_ref[at : at + BLOCK // 2, :] = pieces[2 * d + c][...]
        ctx_ref[d * CTX : (d + 1) * CTX, :] = pieces[2 * d][:CTX, :]
    for i in range(N_Z // 2):
        at = 2 * i * BLOCK
        got = mm(rows_ref[at : at + 2 * BLOCK, :], weight_ref[:, : 3 * LANES]).astype(BF)
        kv_ref[at : at + 2 * BLOCK, :] = got[:, LANES:]
        for k in range(2):
            dest = lax.rem(z_ref[0] - (2 * i + k) + N_Z, N_Z)
            query_ref[dest] = got[k * BLOCK + CTX : (k + 1) * BLOCK, :LANES]
    kvs_ref[...] = mm(ctx_ref[...], weight_ref[:, 4 * LANES :]).astype(BF)


def softmax_rows(query, pairs):
    scores = [mm_nt(query, pair[:, :LANES]) * SCALE for pair in pairs]
    peak = functools.reduce(jnp.maximum, [jnp.max(s, axis=1, keepdims=True) for s in scores])
    total, mixed = (0.0, 0.0)
    for s, pair in zip(scores, pairs):
        raised = jnp.exp(s - peak)
        total = total + jnp.sum(raised, axis=1, keepdims=True)
        mixed = mixed + mm(raised.astype(BF), pair[:, LANES:])
    return mixed / total


def attention_kernel(
    core_ref, query_ref, kv_ref, kv_other_ref, query_s_ref, kvs_ref, kvs_other_ref, listed_ref, out_ref
):
    lane = iota((BLOCK, LANES), 1)

    def one(j, carry):
        pairs = (kv_ref[...], kv_other_ref[...])
        out_ref[j, :TGT, :] = softmax_rows(query_ref[j], pairs).astype(BF)
        at = pl.multiple_of(j * BLOCK, BLOCK)
        pairs = (kvs_ref[...], kvs_other_ref[...])
        mixed = softmax_rows(query_s_ref[pl.ds(at, BLOCK), :], pairs)
        place = (2 * j + core_ref[0]) * BLOCK + iota((BLOCK, listed_ref.shape[1]), 0)
        same = jnp.where(place == listed_ref[...], 1.0, 0.0)
        count = jnp.sum(same, axis=1, keepdims=True)
        out_ref[j, TGT:, :] = jnp.where(lane == HEAD_DIM, count, mixed).astype(BF)
        return carry

    lax.fori_loop(0, N_Z, one, 0)


def output_kernel(
    grp_ref, got_ref, perm_ref, out_ref, student_ref, keep_ref, send_ref, mixed_ref, count_ref,
    wide_ref, thin_ref, part_ref, all_count_ref,
):
    for h in range(N_Z):
        wide_ref[:, h * LANES : (h + 1) * LANES] = got_ref[h, TGT:, :]
        thin_ref[:TGT, h * HEAD_DIM : (h + 1) * HEAD_DIM] = got_ref[h, :TGT, :HEAD_DIM].astype(F32)
    chosen = mm(perm_ref[CTX:, :], wide_ref[...])
    lane = lax.rem(iota(chosen.shape, 1), LANES)
    all_count_ref[...] = jnp.broadcast_to(
        jnp.sum(jnp.where(lane == HEAD_DIM, chosen, 0.0), axis=1, keepdims=True), (TGT, LANES)
    )
    for h in range(N_Z):
        thin_ref[TGT:, h * HEAD_DIM : (h + 1) * HEAD_DIM] = chosen[
            :, h * LANES : h * LANES + HEAD_DIM
        ]
    part_ref[:TGT, :] = mm(thin_ref[:TGT, :].astype(BF), out_ref[...])
    mixed = thin_ref[TGT:, :].astype(BF)
    mixed_ref[...] = mixed
    part_ref[TGT:, :] = mm_nt(mixed, student_ref[...])
    mine = pl.multiple_of(grp_ref[0] * OWN, OWN)
    other = pl.multiple_of((1 - grp_ref[0]) * OWN, OWN)
    keep_ref[:OWN, :] = part_ref[pl.ds(mine, OWN), :].astype(BF)
    keep_ref[OWN:, :] = part_ref[pl.ds(TGT + mine, OWN), :].astype(BF)
    send_ref[:OWN, :] = part_ref[pl.ds(other, OWN), :].astype(BF)
    send_ref[OWN:, :] = part_ref[pl.ds(TGT + other, OWN), :].astype(BF)
    count_ref[...] = all_count_ref[pl.ds(mine, OWN), :]


def slope_kernel(keep_ref, got_ref, tokens_ref, seeds_ref, count_ref, out_ref, back_ref):
    both = keep_ref[...].astype(F32) + got_ref[...].astype(F32)
    wanted = normalized(tokens_ref[...] + both[:OWN])[0].astype(BF).astype(F32)
    predicted, factor = normalized(seeds_ref[...] + both[OWN:])
    slope = jnp.clip(predicted - wanted, -1.0, 1.0) * count_ref[:, :1]
    back_ref[...] = (
        slope
        - jnp.mean(slope, axis=1, keepdims=True)
        - predicted * jnp.mean(slope * predicted, axis=1, keepdims=True)
    ) * factor
    columns = STRIPE * 2 * N_Z
    row = iota((columns, 2 * LANES), 0)
    col = iota((columns, 2 * LANES), 1)
    stripe = lax.div(col, 16)
    inner = lax.rem(col, 16)
    spread = jnp.where((inner < STRIPE) & (row == stripe * STRIPE + inner), 1.0, 0.0).astype(BF)
    for d in range(N_DP):
        part = back_ref[:, d * columns : (d + 1) * columns].astype(BF)
        part = mm(part, spread).astype(BF)
        out_ref[2 * d] = part
        out_ref[2 * d + 1] = part


def finish_kernel(core_ref, mine_ref, other_ref, out_ref):
    total = jnp.zeros(out_ref.shape, F32)
    for ref, flip in ((mine_ref, 0), (other_ref, 1)):
        side = core_ref[0] * (1 - 2 * flip) + flip
        row = iota((out_ref.shape[0], 16 * N_Z), 0)
        col = iota((out_ref.shape[0], 16 * N_Z), 1)
        stripe = side * N_Z + lax.div(col, 16)
        inner = lax.rem(col, 16)
        gather = jnp.where((inner < STRIPE) & (row == stripe * STRIPE + inner), 1.0, 0.0)
        total = total + mm(gather.astype(BF), ref[...])
    out_ref[...] = total


def blend_kernel(target_ref, student_ref, out_ref):
    turned = jnp.transpose(student_ref[...].astype(F32))
    out_ref[...] = MOMENTUM * target_ref[...].astype(F32) + (1.0 - MOMENTUM) * turned


def ring(pieces):
    up = [(i, (i + 1) % N_Z) for i in range(N_Z)]
    down = [(i, (i - 1) % N_Z) for i in range(N_Z)]
    slots = [[None, None] for _ in range(N_Z)]
    slots[0] = list(pieces)
    ups, downs = list(pieces), list(pieces)
    for step in range(1, N_Z // 2 + 1):
        for c in range(2):
            if step < N_Z // 2 or c == 0:
                ups[c] = lax.ppermute(ups[c], "z", up)
                slots[step][c] = ups[c]
            if step < N_Z // 2 or c == 1:
                downs[c] = lax.ppermute(downs[c], "z", down)
                slots[N_Z - step][c] = downs[c]
    return [piece for slot in slots for piece in slot]


def body(
    clips, context, predict_index, target_qkv, target_out, student_qkv, student_out, mask_token
):
    tokens = clips[0]
    width = tokens.shape[1]
    half = width // 2
    z = lax.axis_index("z")
    core = lax.axis_index("core")
    grp = lax.axis_index("grp")
    z_at, core_at, grp_at = (v.astype(I32).reshape(1) for v in (z, core, grp))

    col = jnp.arange(target_qkv.shape[2], dtype=I32)[:, None]
    lane = jnp.arange(LANES, dtype=I32)[None, :]
    picked = ((col == z * HEAD_DIM + lane) & (lane < HEAD_DIM)).astype(BF)
    head = [mm(w[k], picked).astype(BF) for w in (target_qkv, student_qkv) for k in range(3)]
    weights = to_all(jnp.concatenate(head, axis=1), DP, N_DP).reshape(width, 6 * LANES)

    first, second, perm = call(
        sorted_norm_kernel,
        (
            sds((BLOCK // 2, width), BF),
            sds((BLOCK // 2, width), BF),
            sds((BLOCK, BLOCK), BF),
        ),
        name="sorted_norm",
    )(tokens, context)
    pieces = ring((first, second))

    spacing = jnp.exp(jnp.arange(half, dtype=F32) * (-math.log(10000.0) / half))
    spot = jnp.arange(BLOCK, dtype=F32)
    t_angle = spot[:, None] * spacing[None, :]
    base = ((2 * jnp.arange(N_Z, dtype=I32) + core) * BLOCK).astype(F32)
    b_angle = base[:, None] * spacing[None, :]
    listed = predict_index
    listed = jnp.concatenate([listed, lax.ppermute(listed, "core", SWAP)], axis=1)
    rows_own = lax.dynamic_slice_in_dim(perm, CTX + grp * OWN, OWN, axis=0)
    tokens_own = mm(rows_own, tokens)
    places_own = jnp.sum(rows_own.astype(F32) * spot[None, :], axis=1)
    places_own = places_own + ((2 * z + core) * BLOCK).astype(F32)
    angle = places_own[:, None] * spacing[None, :]
    seeds = mask_token[None, :] + jnp.concatenate([jnp.sin(angle), jnp.cos(angle)], axis=1)

    query_s = call(seed_query_kernel, sds((N_Z * BLOCK, LANES), BF), flops=4 * 10**9, name="seed_query")(
        jnp.sin(t_angle),
        jnp.cos(t_angle),
        jnp.sin(b_angle),
        jnp.cos(b_angle),
        mask_token.reshape(2, half),
        weights,
    )

    student_t, weights = lax.optimization_barrier((student_out.T, weights))
    relaid_t = to_all(student_t, DP, N_DP).reshape(width, student_out.shape[0])

    query_t, kv, kvs = call(
        project_kernel,
        (
            sds((N_Z, TGT, LANES), BF),
            sds((N_Z * BLOCK, 2 * LANES), BF),
            sds((N_Z * CTX, 2 * LANES), BF),
        ),
        scratch=(pltpu.VMEM((N_Z * BLOCK, width), BF), pltpu.VMEM((N_Z * CTX, width), BF)),
        in_specs=[SMEM] + [pl.BlockSpec()] * (2 * N_Z + 1),
        flops=2 * 10**9,
        name="project",
    )(z_at, *pieces, weights)
    kv_other = lax.ppermute(kv, "core", SWAP)
    kvs_other = lax.ppermute(kvs, "core", SWAP)
    mixed = call(
        attention_kernel,
        sds((N_Z, TGT + BLOCK, LANES), BF),
        in_specs=[SMEM] + [pl.BlockSpec()] * 7,
        flops=4 * 10**9,
        name="attention",
    )(core_at, query_t, kv, kv_other, query_s, kvs, kvs_other, listed)
    mixed = lax.all_to_all(mixed, "z", split_axis=0, concat_axis=0, tiled=True)

    keep, send, mixed_c, count = call(
        output_kernel,
        (
            sds((2 * OWN, width), BF),
            sds((2 * OWN, width), BF),
            sds((TGT, N_Z * HEAD_DIM), BF),
            sds((OWN, LANES), F32),
        ),
        scratch=(
            pltpu.VMEM((BLOCK, N_Z * LANES), BF),
            pltpu.VMEM((2 * TGT, N_Z * HEAD_DIM), F32),
            pltpu.VMEM((2 * TGT, width), F32),
            pltpu.VMEM((TGT, LANES), F32),
        ),
        in_specs=[SMEM] + [pl.BlockSpec()] * 4,
        flops=10**9,
        name="output",
    )(grp_at, mixed, perm, target_out, relaid_t)
    got = lax.ppermute(send, "grp", SWAP)
    mixed_all = to_all(mixed_c, DP, N_DP).reshape(N_DP * TGT, N_Z * HEAD_DIM)
    got, mixed_all = lax.optimization_barrier((got, mixed_all))
    stripes = call(
        slope_kernel,
        sds((2 * N_DP, OWN, 256), BF),
        scratch=(pltpu.VMEM((OWN, width), F32),),
        name="slope",
    )(keep, got, tokens_own, seeds, count)
    arrived = lax.all_to_all(stripes, (*DP, "grp"), split_axis=0, concat_axis=0, tiled=True)
    grad = lax.dot_general(
        arrived.reshape(N_DP * TGT, 256),
        mixed_all,
        (((0,), (0,)), ((), ())),
        preferred_element_type=F32,
    )
    lower, upper = (grad[: 16 * N_Z], grad[16 * N_Z :])
    grad_keep = jnp.where(core == 0, lower, upper)
    grad_send = jnp.where(core == 0, upper, lower)
    grad = grad_keep + lax.ppermute(grad_send, "core", SWAP)
    grad = grad.astype(BF).reshape(N_Z, 16, N_Z * HEAD_DIM)
    grad = lax.all_to_all(grad, "z", split_axis=0, concat_axis=0, tiled=True)
    grad = jnp.sum(grad.astype(F32), axis=0).astype(BF)
    grad = to_all(grad, "z", N_Z).reshape(16 * N_Z, N_Z * HEAD_DIM)
    other = lax.ppermute(grad, "core", SWAP)
    out_grad = call(
        finish_kernel,
        sds((student_out.shape[1], student_out.shape[0]), F32),
        in_specs=[SMEM] + [pl.BlockSpec()] * 2,
        name="finish",
    )(core_at, grad, other).T

    target_blend = pl.pallas_call(
        blend_kernel,
        grid=(width // LANES,),
        in_specs=[
            pl.BlockSpec((half, LANES), lambda i: (0, i)),
            pl.BlockSpec((LANES, half), lambda i: (i, 0)),
        ],
        out_specs=pl.BlockSpec((half, LANES), lambda i: (0, i)),
        out_shape=sds((half, width), F32),
        cost_estimate=pl.CostEstimate(flops=4 * 10**9, bytes_accessed=10**7, transcendentals=0),
        name="blend",
    )(target_out, relaid_t)
    return (out_grad, target_blend)


def solution(mesh):
    fine = Mesh(mesh.devices.reshape(8, 2, 2, 2, 4), ("z", "core", "grp", "ylo", "x"))
    seq = ("z", "core")
    in_specs = (
        P(DP, seq, None),
        P(DP, seq),
        P(DP, seq),
        P(None, DP, "grp"),
        P("grp", None),
        P(None, DP, "grp"),
        P("grp", DP),
        P(),
    )
    out_specs = (P("grp", DP), P("grp", None))
    return jax.shard_map(body, mesh=fine, in_specs=in_specs, out_specs=out_specs, check_vma=False)
```

```python
import functools
import math

import jax
import jax.numpy as jnp
from jax import lax
from jax.experimental import pallas as pl
from jax.experimental.pallas import tpu as pltpu
from jax.sharding import Mesh, PartitionSpec as P


HEAD_DIM = 88
LANES = 128
CTX = 32
BLOCK = 128
TGT = 96
OWN = 48
N_Z = 8
N_DP = 8
STRIPE = 11
EPSILON = 1e-06
MOMENTUM = 0.99
SCALE = HEAD_DIM ** (-0.5)
BF = jnp.bfloat16
F32 = jnp.float32
I32 = jnp.int32
SWAP = [(0, 1), (1, 0)]
FLOPS = 10**6
DP = ("ylo", "x")
SMEM = pl.BlockSpec(memory_space=pltpu.SMEM)


def iota(shape, dim):
    return lax.broadcasted_iota(I32, shape, dim)


def mm(a, b):
    return jnp.dot(a, b, preferred_element_type=F32)


def mm_nt(a, b):
    return lax.dot_general(a, b, (((1,), (1,)), ((), ())), preferred_element_type=F32)


def sds(shape, dtype):
    return jax.ShapeDtypeStruct(shape, dtype)


def call(kernel, outs, scratch=(), flops=FLOPS, **specs):
    return pl.pallas_call(
        kernel,
        out_shape=outs,
        scratch_shapes=list(scratch),
        **specs,
        cost_estimate=pl.CostEstimate(flops=flops, bytes_accessed=10**6, transcendentals=0),
    )


def to_all(shard, axes, count):
    copies = jnp.broadcast_to(shard[None], (count, *shard.shape))
    return lax.all_to_all(copies, axes, split_axis=0, concat_axis=0, tiled=True)


def exchange(pieces, axes):
    return lax.all_to_all(pieces, axes, split_axis=0, concat_axis=0, tiled=True)


def after(value, others):
    return lax.optimization_barrier((value, others))[0]


def normalized(values):
    center = values - jnp.mean(values, axis=-1, keepdims=True)
    factor = lax.rsqrt(jnp.mean(center * center, axis=-1, keepdims=True) + EPSILON)
    return (center * factor, factor)


def sorted_norm_kernel(tokens_ref, context_ref, moved_ref, perm_ref):
    normed = normalized(tokens_ref[...].astype(F32))[0].astype(BF)
    flag = jnp.where(context_ref[...] == 1, 1.0, 0.0)
    upto = jnp.where(iota((BLOCK, BLOCK), 0) <= iota((BLOCK, BLOCK), 1), 1.0, 0.0).astype(BF)
    before = mm(jnp.broadcast_to(flag, (16, BLOCK)).astype(BF), upto)[:1]
    spot = iota((1, BLOCK), 1).astype(F32)
    rank = jnp.where(flag == 1.0, before - 1.0, CTX + spot - before).astype(I32)
    perm = jnp.where(rank == iota((BLOCK, BLOCK), 0), 1.0, 0.0).astype(BF)
    moved_ref[...] = mm(perm, normed).astype(BF)
    perm_ref[...] = perm


def head_kernel(z_ref, core_ref, target_ref, student_ref, out_ref):
    rows = target_ref.shape[2]
    col = z_ref[0] * HEAD_DIM + iota((rows, LANES), 1)
    same = (iota((rows, LANES), 0) == col) & (iota((rows, LANES), 1) < HEAD_DIM)
    picked = jnp.where(same, 1.0, 0.0).astype(BF)

    def fill(ref):
        for k in range(3):
            got = mm(ref[k], picked).astype(BF)
            for d in range(N_DP):
                out_ref[d, :, k * LANES : (k + 1) * LANES] = got

    pl.when(core_ref[0] == 0)(lambda: fill(target_ref))
    pl.when(core_ref[0] == 1)(lambda: fill(student_ref))


def seed_norm_kernel(sin_ref, cos_ref, bsin_ref, bcos_ref, mask_ref, lower_ref, upper_ref):
    half = sin_ref.shape[1]
    rows = 32
    bsin = bsin_ref[0]
    bcos = bcos_ref[0]

    def one(i, carry):
        at = pl.multiple_of(i * rows, rows)
        t_sin = sin_ref[pl.ds(at, rows), :]
        t_cos = cos_ref[pl.ds(at, rows), :]
        a = bsin * t_cos + bcos * t_sin + mask_ref[0:1, :]
        b = bcos * t_cos - bsin * t_sin + mask_ref[1:2, :]
        mean = (jnp.sum(a, -1, keepdims=True) + jnp.sum(b, -1, keepdims=True)) / (2 * half)
        a = a - mean
        b = b - mean
        var = (jnp.sum(a * a, -1, keepdims=True) + jnp.sum(b * b, -1, keepdims=True)) / (2 * half)
        inv = lax.rsqrt(var + EPSILON)
        lower_ref[pl.ds(at, rows), :] = (a * inv).astype(BF)
        upper_ref[pl.ds(at, rows), :] = (b * inv).astype(BF)
        return carry

    lax.fori_loop(0, BLOCK // rows, one, 0, unroll=2)


def project_kernel(z_ref, *refs):
    pieces = refs[: N_Z - 1]
    target_ref, student_ref, query_ref, kv_ref, kvs_ref, rows_ref, ctx_ref = refs[N_Z - 1 :]
    slots = [d for d in range(N_Z) if d != N_Z // 2]
    for i in range(N_Z - 1):
        rows_ref[i * BLOCK : (i + 1) * BLOCK, :] = pieces[i][...]
        ctx_ref[i * CTX : (i + 1) * CTX, :] = pieces[i][:CTX, :]
    for at, count in ((0, 2), (2, 2), (4, 2), (6, 1)):
        rows = slice(at * BLOCK, (at + count) * BLOCK)
        got = mm(rows_ref[rows, :], target_ref[...]).astype(BF)
        kv_ref[rows, :] = got[:, LANES:]
        for k in range(count):
            dest = lax.rem(z_ref[0] - slots[at + k] + N_Z, N_Z)
            query_ref[dest] = got[k * BLOCK + CTX : (k + 1) * BLOCK, :LANES]
    kvs_ref[...] = mm(ctx_ref[...], student_ref[:, LANES:]).astype(BF)


def project_last_kernel(
    first_ref, second_ref, kvs_early_ref, target_ref, student_ref, query_ref, kv_ref, kvs_ref, rows_ref
):
    early = (N_Z - 1) * CTX
    kvs_ref[:early, :] = kvs_early_ref[...]
    kvs_ref[early:, :] = mm(first_ref[:CTX, :], student_ref[:, LANES:]).astype(BF)
    rows_ref[: BLOCK // 2, :] = first_ref[...]
    rows_ref[BLOCK // 2 :, :] = second_ref[...]
    got = mm(rows_ref[...], target_ref[...]).astype(BF)
    kv_ref[...] = got[:, LANES:]
    query_ref[...] = got[CTX:, :LANES]


def softmax_rows(query, pairs):
    scores = [mm_nt(query, pair[:, :LANES]) * SCALE for pair in pairs]
    peak = functools.reduce(jnp.maximum, [jnp.max(s, axis=1, keepdims=True) for s in scores])
    total, mixed = (0.0, 0.0)
    for s, pair in zip(scores, pairs):
        raised = jnp.exp(s - peak)
        total = total + jnp.sum(raised, axis=1, keepdims=True)
        mixed = mixed + mm(raised.astype(BF), pair[:, LANES:])
    return mixed / total


def attend_target_kernel(
    z_ref, query_ref, query_last_ref, kv_ref, kv_other_ref, last_ref, last_other_ref, out_ref
):
    last = lax.rem(z_ref[0] + N_Z // 2, N_Z)

    def one(j, carry):
        query = jnp.where(j == last, query_last_ref[...], query_ref[j])
        pairs = (kv_ref, kv_other_ref, last_ref, last_other_ref)
        out_ref[j] = softmax_rows(query, [pair[...] for pair in pairs]).astype(BF)
        return carry

    lax.fori_loop(0, N_Z, one, 0)


def attend_student_kernel(core_ref, query_ref, kvs_ref, kvs_other_ref, listed_ref, out_ref):
    lane = iota((BLOCK, LANES), 1)

    def one(j, carry):
        at = pl.multiple_of(j * BLOCK, BLOCK)
        pairs = (kvs_ref[...], kvs_other_ref[...])
        mixed = softmax_rows(query_ref[pl.ds(at, BLOCK), :], pairs)
        place = (2 * j + core_ref[0]) * BLOCK + iota((BLOCK, listed_ref.shape[1]), 0)
        same = jnp.where(place == listed_ref[...], 1.0, 0.0)
        count = jnp.sum(same, axis=1, keepdims=True)
        out_ref[j] = jnp.where(lane == HEAD_DIM, count, mixed).astype(BF)
        return carry

    lax.fori_loop(0, N_Z, one, 0)


def divide(grp_ref, part_ref, keep_ref, send_ref):
    mine = pl.multiple_of(grp_ref[0] * OWN, OWN)
    other = pl.multiple_of((1 - grp_ref[0]) * OWN, OWN)
    keep_ref[...] = part_ref[pl.ds(mine, OWN), :].astype(BF)
    send_ref[...] = part_ref[pl.ds(other, OWN), :].astype(BF)


def output_student_kernel(
    grp_ref, got_ref, perm_ref, student_ref, keep_ref, send_ref, mixed_ref, count_ref,
    wide_ref, thin_ref, part_ref, all_count_ref,
):
    for h in range(N_Z):
        wide_ref[:, h * LANES : (h + 1) * LANES] = got_ref[h]
    chosen = mm(perm_ref[CTX:, :], wide_ref[...])
    lane = lax.rem(iota(chosen.shape, 1), LANES)
    all_count_ref[...] = jnp.broadcast_to(
        jnp.sum(jnp.where(lane == HEAD_DIM, chosen, 0.0), axis=1, keepdims=True), (TGT, LANES)
    )
    for h in range(N_Z):
        thin_ref[:, h * HEAD_DIM : (h + 1) * HEAD_DIM] = chosen[:, h * LANES : h * LANES + HEAD_DIM]
    mixed = thin_ref[...].astype(BF)
    for d in range(N_DP):
        mixed_ref[d] = mixed
    part_ref[...] = mm_nt(mixed, student_ref[...])
    divide(grp_ref, part_ref, keep_ref, send_ref)
    count_ref[...] = all_count_ref[pl.ds(pl.multiple_of(grp_ref[0] * OWN, OWN), OWN), :]


def output_target_kernel(grp_ref, got_ref, out_ref, keep_ref, send_ref, thin_ref, part_ref):
    for h in range(N_Z):
        thin_ref[:, h * HEAD_DIM : (h + 1) * HEAD_DIM] = got_ref[h, :, :HEAD_DIM].astype(F32)
    part_ref[...] = mm(thin_ref[...].astype(BF), out_ref[...])
    divide(grp_ref, part_ref, keep_ref, send_ref)


def slope_kernel(
    keep_ref, got_ref, keep_s_ref, got_s_ref, tokens_ref, seeds_ref, count_ref, out_ref, back_ref
):
    target_sum = keep_ref[...].astype(F32) + got_ref[...].astype(F32)
    student_sum = keep_s_ref[...].astype(F32) + got_s_ref[...].astype(F32)
    wanted = normalized(tokens_ref[...] + target_sum)[0].astype(BF).astype(F32)
    predicted, factor = normalized(seeds_ref[...] + student_sum)
    slope = jnp.clip(predicted - wanted, -1.0, 1.0) * count_ref[:, :1]
    back_ref[...] = (
        slope
        - jnp.mean(slope, axis=1, keepdims=True)
        - predicted * jnp.mean(slope * predicted, axis=1, keepdims=True)
    ) * factor
    columns = STRIPE * 2 * N_Z
    row = iota((columns, 2 * LANES), 0)
    col = iota((columns, 2 * LANES), 1)
    stripe = lax.div(col, 16)
    inner = lax.rem(col, 16)
    spread = jnp.where((inner < STRIPE) & (row == stripe * STRIPE + inner), 1.0, 0.0).astype(BF)
    for d in range(N_DP):
        part = back_ref[:, d * columns : (d + 1) * columns].astype(BF)
        part = mm(part, spread).astype(BF)
        out_ref[2 * d] = part
        out_ref[2 * d + 1] = part


def finish_kernel(core_ref, mine_ref, other_ref, out_ref):
    total = jnp.zeros(out_ref.shape, F32)
    for ref, flip in ((mine_ref, 0), (other_ref, 1)):
        side = core_ref[0] * (1 - 2 * flip) + flip
        row = iota((out_ref.shape[0], 16 * N_Z), 0)
        col = iota((out_ref.shape[0], 16 * N_Z), 1)
        stripe = side * N_Z + lax.div(col, 16)
        inner = lax.rem(col, 16)
        gather = jnp.where((inner < STRIPE) & (row == stripe * STRIPE + inner), 1.0, 0.0)
        total = total + mm(gather.astype(BF), ref[...])
    out_ref[...] = total


def blend_kernel(target_ref, student_ref, out_ref):
    turned = jnp.transpose(student_ref[...].astype(F32))
    out_ref[...] = MOMENTUM * target_ref[...].astype(F32) + (1.0 - MOMENTUM) * turned


def ring(rows, gates):
    up = [(i, (i + 1) % N_Z) for i in range(N_Z)]
    down = [(i, (i - 1) % N_Z) for i in range(N_Z)]
    below = above = rows
    lower, upper = ([], [])
    for step in range(1, N_Z // 2):
        if step in gates:
            below, above, _ = lax.optimization_barrier((below, above, gates[step]))
        below = lax.ppermute(below, "z", up)
        above = lax.ppermute(above, "z", down)
        lower.append(below)
        upper.append(above)
    first = lax.ppermute(below[: BLOCK // 2], "z", up)
    second = lax.ppermute(above[BLOCK // 2 :], "z", down)
    return [rows] + lower + upper[::-1], (first, second)


def body(
    clips, context, predict_index, target_qkv, target_out, student_qkv, student_out, mask_token
):
    tokens = clips[0]
    width = tokens.shape[1]
    half = width // 2
    z = lax.axis_index("z")
    core = lax.axis_index("core")
    grp = lax.axis_index("grp")
    z_at, core_at, grp_at = (v.astype(I32).reshape(1) for v in (z, core, grp))

    moved, perm = call(
        sorted_norm_kernel, (sds((BLOCK, width), BF), sds((BLOCK, BLOCK), BF))
    )(tokens, context)
    spacing = jnp.exp(jnp.arange(half, dtype=F32) * (-math.log(10000.0) / half))
    spot = jnp.arange(BLOCK, dtype=F32)
    t_angle = spot[:, None] * spacing[None, :]
    base = ((2 * jnp.arange(N_Z, dtype=I32) + core) * BLOCK).astype(F32)
    b_angle = base[:, None] * spacing[None, :]
    tables = (
        jnp.sin(t_angle),
        jnp.cos(t_angle),
        jnp.sin(b_angle)[:, None],
        jnp.cos(b_angle)[:, None],
    )
    table = pl.BlockSpec((BLOCK, half), lambda j: (0, 0))
    row = pl.BlockSpec((1, 1, half), lambda j: (j, 0, 0))
    block = pl.BlockSpec((BLOCK, half), lambda j: (j, 0))
    seed_a, seed_b = call(
        seed_norm_kernel,
        (sds((N_Z * BLOCK, half), BF), sds((N_Z * BLOCK, half), BF)),
        grid=(N_Z,),
        in_specs=[table, table, row, row, pl.BlockSpec((2, half), lambda j: (0, 0))],
        out_specs=(block, block),
    )(
        *tables,
        mask_token.reshape(2, half),
    )
    pieces, last = ring(moved, {2: tables, 3: (seed_a, seed_b)})

    head = call(
        head_kernel,
        sds((N_DP, width // N_DP, 3 * LANES), BF),
        in_specs=[SMEM, SMEM, pl.BlockSpec(), pl.BlockSpec()],
    )(z_at, core_at, after(target_qkv, moved), student_qkv)
    weights = after(exchange(head, DP), seed_a).reshape(width, 3 * LANES)
    swapped = lax.ppermute(weights, "core", SWAP)
    target_w = jnp.where(core == 0, weights, swapped)
    student_w = jnp.where(core == 0, swapped, weights)

    cols = student_out.shape[1] // 2
    turned = lax.dynamic_slice_in_dim(student_out.T, core * cols, cols, axis=0)
    fetched = to_all(after(turned, weights), DP, N_DP)
    fetched_other = lax.ppermute(fetched, "core", SWAP)
    relaid_t = jnp.where(
        core == 0,
        jnp.stack([fetched, fetched_other], axis=1),
        jnp.stack([fetched_other, fetched], axis=1),
    ).reshape(width, student_out.shape[0])

    listed = predict_index
    listed = jnp.concatenate([listed, lax.ppermute(listed, "core", SWAP)], axis=1)
    rows_own = lax.dynamic_slice_in_dim(perm, CTX + grp * OWN, OWN, axis=0)
    tokens_own = mm(rows_own, tokens)
    places_own = jnp.sum(rows_own.astype(F32) * spot[None, :], axis=1)
    places_own = places_own + ((2 * z + core) * BLOCK).astype(F32)
    angle = places_own[:, None] * spacing[None, :]
    seeds = mask_token[None, :] + jnp.concatenate([jnp.sin(angle), jnp.cos(angle)], axis=1)

    query_s = mm(seed_a, student_w[:half, :LANES]) + mm(seed_b, student_w[half:, :LANES])
    query_s = query_s.astype(BF)

    query_t, kv, kvs = call(
        project_kernel,
        (
            sds((N_Z, TGT, LANES), BF),
            sds(((N_Z - 1) * BLOCK, 2 * LANES), BF),
            sds(((N_Z - 1) * CTX, 2 * LANES), BF),
        ),
        scratch=(
            pltpu.VMEM(((N_Z - 1) * BLOCK, width), BF),
            pltpu.VMEM(((N_Z - 1) * CTX, width), BF),
        ),
        in_specs=[SMEM] + [pl.BlockSpec()] * (N_Z + 1),
    )(z_at, *pieces, target_w, student_w)
    kv_other = lax.ppermute(kv, "core", SWAP)
    query_last, kv_last, kvs = call(
        project_last_kernel,
        (
            sds((TGT, LANES), BF),
            sds((BLOCK, 2 * LANES), BF),
            sds((N_Z * CTX, 2 * LANES), BF),
        ),
        scratch=(pltpu.VMEM((BLOCK, width), BF),),
    )(*last, kvs, target_w, student_w)
    kvs_other = lax.ppermute(kvs, "core", SWAP)
    kv_last_other = lax.ppermute(kv_last, "core", SWAP)

    mixed_s = call(
        attend_student_kernel, sds((N_Z, BLOCK, LANES), BF), in_specs=[SMEM] + [pl.BlockSpec()] * 4
    )(core_at, query_s, kvs, kvs_other, listed)
    mixed_s = exchange(after(mixed_s, relaid_t), "z")
    mixed_t = call(
        attend_target_kernel, sds((N_Z, TGT, LANES), BF), in_specs=[SMEM] + [pl.BlockSpec()] * 6
    )(z_at, query_t, query_last, kv, kv_other, kv_last, kv_last_other)
    mixed_t = exchange(after(mixed_t, mixed_s), "z")
    keep_s, send_s, mixed_c, count = call(
        output_student_kernel,
        (
            sds((OWN, width), BF),
            sds((OWN, width), BF),
            sds((N_DP, TGT, N_Z * HEAD_DIM), BF),
            sds((OWN, LANES), F32),
        ),
        scratch=(
            pltpu.VMEM((BLOCK, N_Z * LANES), BF),
            pltpu.VMEM((TGT, N_Z * HEAD_DIM), F32),
            pltpu.VMEM((TGT, width), F32),
            pltpu.VMEM((TGT, LANES), F32),
        ),
        in_specs=[SMEM] + [pl.BlockSpec()] * 3,
    )(grp_at, mixed_s, perm, relaid_t)
    got_s = lax.ppermute(send_s, "grp", SWAP)
    target_blend = call(
        blend_kernel,
        sds((half, width), F32),
        grid=(width // LANES,),
        in_specs=[
            pl.BlockSpec((half, LANES), lambda i: (0, i)),
            pl.BlockSpec((LANES, half), lambda i: (i, 0)),
        ],
        out_specs=pl.BlockSpec((half, LANES), lambda i: (0, i)),
    )(target_out, after(relaid_t, mixed_c))
    keep, send = call(
        output_target_kernel,
        (sds((OWN, width), BF), sds((OWN, width), BF)),
        scratch=(pltpu.VMEM((TGT, N_Z * HEAD_DIM), F32), pltpu.VMEM((TGT, width), F32)),
        in_specs=[SMEM] + [pl.BlockSpec()] * 2,
    )(grp_at, after(mixed_t, got_s), target_out)
    got = lax.ppermute(send, "grp", SWAP)
    mixed_all = exchange(after(mixed_c, (mixed_t, target_blend)), DP).reshape(N_DP * TGT, N_Z * HEAD_DIM)
    stripes = call(
        slope_kernel, sds((2 * N_DP, OWN, 256), BF), scratch=(pltpu.VMEM((OWN, width), F32),)
    )(keep, got, keep_s, got_s, tokens_own, seeds, count)
    stripes = after(stripes, mixed_all)
    arrived = lax.all_to_all(stripes, (*DP, "grp"), split_axis=0, concat_axis=0, tiled=True)
    grad = lax.dot_general(
        arrived.reshape(N_DP * TGT, 256),
        mixed_all,
        (((0,), (0,)), ((), ())),
        preferred_element_type=F32,
    )
    lower, upper = (grad[: 16 * N_Z], grad[16 * N_Z :])
    grad_keep = jnp.where(core == 0, lower, upper)
    grad_send = jnp.where(core == 0, upper, lower)
    grad = grad_keep + lax.ppermute(grad_send, "core", SWAP)
    grad = grad.astype(BF).reshape(N_Z, 16, N_Z * HEAD_DIM)
    grad = lax.all_to_all(grad, "z", split_axis=0, concat_axis=0, tiled=True)
    grad = jnp.sum(grad.astype(F32), axis=0).astype(BF)
    grad = to_all(grad, "z", N_Z).reshape(16 * N_Z, N_Z * HEAD_DIM)
    other = lax.ppermute(grad, "core", SWAP)
    out_grad = call(
        finish_kernel,
        sds((student_out.shape[1], student_out.shape[0]), F32),
        in_specs=[SMEM] + [pl.BlockSpec()] * 2,
    )(core_at, grad, other).T
    return (out_grad, target_blend)


def solution(mesh):
    fine = Mesh(mesh.devices.reshape(8, 2, 2, 2, 4), ("z", "core", "grp", "ylo", "x"))
    seq = ("z", "core")
    in_specs = (
        P(DP, seq, None),
        P(DP, seq),
        P(DP, seq),
        P(None, DP, "grp"),
        P("grp", None),
        P(None, DP, "grp"),
        P("grp", DP),
        P(),
    )
    out_specs = (P("grp", DP), P("grp", None))
    return jax.shard_map(body, mesh=fine, in_specs=in_specs, out_specs=out_specs, check_vma=False)
```

```python
import functools
import math

import jax
import jax.numpy as jnp
from jax import lax
from jax.experimental import pallas as pl
from jax.experimental.pallas import tpu as pltpu
from jax.sharding import Mesh, PartitionSpec as P


HEAD_DIM = 88
LANES = 128
WIDE = 384
CTX = 32
BLOCK = 128
TGT = 96
OWN = 48
N_Z = 8
N_DP = 8
STRIPE = 11
EPSILON = 1e-06
MOMENTUM = 0.99
SCALE = HEAD_DIM ** (-0.5)
BF = jnp.bfloat16
F32 = jnp.float32
I32 = jnp.int32
SWAP = [(0, 1), (1, 0)]
FLOPS = 10**6
DP = ("ylo", "x")
SMEM = pl.BlockSpec(memory_space=pltpu.SMEM)


def iota(shape, dim):
    return lax.broadcasted_iota(I32, shape, dim)


def mm(a, b):
    return jnp.dot(a, b, preferred_element_type=F32)


def mm_nt(a, b):
    return lax.dot_general(a, b, (((1,), (1,)), ((), ())), preferred_element_type=F32)


def sds(shape, dtype):
    return jax.ShapeDtypeStruct(shape, dtype)


def call(kernel, outs, scratch=(), flops=FLOPS, **specs):
    return pl.pallas_call(
        kernel,
        out_shape=outs,
        scratch_shapes=list(scratch),
        **specs,
        cost_estimate=pl.CostEstimate(flops=flops, bytes_accessed=10**6, transcendentals=0),
    )


def to_all(shard, axes, count):
    copies = jnp.broadcast_to(shard[None], (count, *shard.shape))
    return lax.all_to_all(copies, axes, split_axis=0, concat_axis=0, tiled=True)


def exchange(pieces, axes):
    return lax.all_to_all(pieces, axes, split_axis=0, concat_axis=0, tiled=True)


def after(value, others):
    return lax.optimization_barrier((value, others))[0]


def normalized(values):
    center = values - jnp.mean(values, axis=-1, keepdims=True)
    factor = lax.rsqrt(jnp.mean(center * center, axis=-1, keepdims=True) + EPSILON)
    return (center * factor, factor)


def sorted_norm_kernel(tokens_ref, context_ref, moved_ref, perm_ref):
    normed = normalized(tokens_ref[...].astype(F32))[0].astype(BF)
    flag = jnp.where(context_ref[...] == 1, 1.0, 0.0)
    upto = jnp.where(iota((BLOCK, BLOCK), 0) <= iota((BLOCK, BLOCK), 1), 1.0, 0.0).astype(BF)
    before = mm(jnp.broadcast_to(flag, (16, BLOCK)).astype(BF), upto)[:1]
    spot = iota((1, BLOCK), 1).astype(F32)
    rank = jnp.where(flag == 1.0, before - 1.0, CTX + spot - before).astype(I32)
    perm = jnp.where(rank == iota((BLOCK, BLOCK), 0), 1.0, 0.0).astype(BF)
    moved_ref[...] = mm(perm, normed).astype(BF)
    perm_ref[...] = perm


def head_kernel(z_ref, core_ref, target_ref, student_ref, turned_ref, out_ref):
    rows = target_ref.shape[2]
    half = turned_ref.shape[1] // 2
    col = z_ref[0] * HEAD_DIM + iota((rows, LANES), 1)
    same = (iota((rows, LANES), 0) == col) & (iota((rows, LANES), 1) < HEAD_DIM)
    picked = jnp.where(same, 1.0, 0.0).astype(BF)

    def fill(ref, at):
        got = [mm(ref[k], picked).astype(BF) for k in range(3)]
        turned = turned_ref[:, at : at + half]
        rest = jnp.zeros((turned.shape[0], WIDE - half), BF)
        for d in range(N_DP):
            for k in range(3):
                out_ref[d, :, k * LANES : (k + 1) * LANES] = got[k]
            out_ref[d, :, WIDE : WIDE + half] = turned
            out_ref[d, :, WIDE + half :] = rest

    pl.when(core_ref[0] == 0)(lambda: fill(target_ref, 0))
    pl.when(core_ref[0] == 1)(lambda: fill(student_ref, half))


def seed_norm_kernel(sin_ref, cos_ref, bsin_ref, bcos_ref, mask_ref, lower_ref, upper_ref):
    half = sin_ref.shape[1]
    rows = 32
    bsin = bsin_ref[pl.ds(pl.program_id(0), 1), :]
    bcos = bcos_ref[pl.ds(pl.program_id(0), 1), :]

    def one(i, carry):
        at = pl.multiple_of(i * rows, rows)
        t_sin = sin_ref[pl.ds(at, rows), :]
        t_cos = cos_ref[pl.ds(at, rows), :]
        a = bsin * t_cos + bcos * t_sin + mask_ref[0:1, :]
        b = bcos * t_cos - bsin * t_sin + mask_ref[1:2, :]
        mean = (jnp.sum(a, -1, keepdims=True) + jnp.sum(b, -1, keepdims=True)) / (2 * half)
        a = a - mean
        b = b - mean
        var = (jnp.sum(a * a, -1, keepdims=True) + jnp.sum(b * b, -1, keepdims=True)) / (2 * half)
        inv = lax.rsqrt(var + EPSILON)
        lower_ref[pl.ds(at, rows), :] = (a * inv).astype(BF)
        upper_ref[pl.ds(at, rows), :] = (b * inv).astype(BF)
        return carry

    lax.fori_loop(0, BLOCK // rows, one, 0, unroll=2)


def seed_query_kernel(core_ref, lower_ref, upper_ref, mine_ref, other_ref, out_ref):
    half = lower_ref.shape[1]
    weight = jnp.where(core_ref[0] == 1, mine_ref[...], other_ref[...])
    query = mm(lower_ref[...], weight[:half]) + mm(upper_ref[...], weight[half:])
    out_ref[...] = query.astype(BF)


def project_kernel(z_ref, core_ref, *refs):
    pieces = refs[:N_Z]
    mine_ref, other_ref, query_ref, kv_ref, kvs_ref, rows_ref, ctx_ref, target_ref = refs[N_Z:]
    for i in range(N_Z):
        rows_ref[i * BLOCK : (i + 1) * BLOCK, :] = pieces[i][...]
        ctx_ref[i * CTX : (i + 1) * CTX, :] = pieces[i][:CTX, :]
    target_ref[...] = jnp.where(core_ref[0] == 0, mine_ref[...], other_ref[...])
    student = jnp.where(core_ref[0] == 0, other_ref[:, LANES:], mine_ref[:, LANES:])
    kvs_ref[...] = mm(ctx_ref[...], student).astype(BF)
    for i in range(2):
        rows = slice(i * 4 * BLOCK, (i + 1) * 4 * BLOCK)
        got = mm(rows_ref[rows, :], target_ref[...]).astype(BF)
        kv_ref[rows, :] = got[:, LANES:]
        for k in range(4):
            dest = lax.rem(z_ref[0] - (4 * i + k) + N_Z, N_Z)
            query_ref[dest] = got[k * BLOCK + CTX : (k + 1) * BLOCK, :LANES]


def softmax_rows(query, pairs):
    scores = [mm_nt(query, pair[:, :LANES]) * SCALE for pair in pairs]
    peak = functools.reduce(jnp.maximum, [jnp.max(s, axis=1, keepdims=True) for s in scores])
    total, mixed = (0.0, 0.0)
    for s, pair in zip(scores, pairs):
        raised = jnp.exp(s - peak)
        total = total + jnp.sum(raised, axis=1, keepdims=True)
        mixed = mixed + mm(raised.astype(BF), pair[:, LANES:])
    return mixed / total


def attend_target_kernel(query_ref, kv_ref, kv_other_ref, out_ref):
    rows = 4 * TGT
    for i in range(2):
        query = query_ref[4 * i : 4 * i + 4].reshape(rows, LANES)
        mixed = softmax_rows(query, (kv_ref, kv_other_ref)).astype(BF)
        out_ref[4 * i : 4 * i + 4] = mixed.reshape(4, TGT, LANES)


def attend_student_kernel(core_ref, query_ref, kvs_ref, kvs_other_ref, listed_ref, out_ref):
    rows = 4 * BLOCK
    lane = iota((rows, LANES), 1)
    slot = iota((rows, listed_ref.shape[1]), 0)
    for i in range(2):
        mixed = softmax_rows(query_ref[i * rows : (i + 1) * rows, :], (kvs_ref, kvs_other_ref))
        block = lax.div(slot, BLOCK)
        place = (2 * (4 * i + block) + core_ref[0]) * BLOCK + slot - block * BLOCK
        same = jnp.where(place == listed_ref[...], 1.0, 0.0)
        count = jnp.sum(same, axis=1, keepdims=True)
        mixed = jnp.where(lane == HEAD_DIM, count, mixed).astype(BF)
        out_ref[4 * i : 4 * i + 4] = mixed.reshape(4, BLOCK, LANES)


def divide(grp_ref, part_ref, keep_ref, send_ref):
    mine = pl.multiple_of(grp_ref[0] * OWN, OWN)
    other = pl.multiple_of((1 - grp_ref[0]) * OWN, OWN)
    keep_ref[...] = part_ref[pl.ds(mine, OWN), :].astype(BF)
    send_ref[...] = part_ref[pl.ds(other, OWN), :].astype(BF)


def output_student_kernel(
    grp_ref, core_ref, got_ref, perm_ref, mine_ref, other_ref, keep_ref, send_ref, mixed_ref,
    count_ref, wide_ref, thin_ref, part_ref, all_count_ref,
):
    for h in range(N_Z):
        wide_ref[:, h * LANES : (h + 1) * LANES] = got_ref[h]
    chosen = mm(perm_ref[CTX:, :], wide_ref[...])
    lane = lax.rem(iota(chosen.shape, 1), LANES)
    all_count_ref[...] = jnp.broadcast_to(
        jnp.sum(jnp.where(lane == HEAD_DIM, chosen, 0.0), axis=1, keepdims=True), (TGT, LANES)
    )
    thin_ref[...] = jnp.zeros(thin_ref.shape, F32)
    for h in range(N_Z):
        at = (h // 4) * WIDE + (h % 4) * HEAD_DIM
        thin_ref[:, at : at + HEAD_DIM] = chosen[:, h * LANES : h * LANES + HEAD_DIM]
    mixed = thin_ref[...].astype(BF)
    for d in range(N_DP):
        mixed_ref[d] = mixed
    left = jnp.where(core_ref[0] == 0, mine_ref[...], other_ref[...])
    right = jnp.where(core_ref[0] == 0, other_ref[...], mine_ref[...])
    part_ref[...] = mm_nt(mixed[:, :WIDE], left) + mm_nt(mixed[:, WIDE:], right)
    divide(grp_ref, part_ref, keep_ref, send_ref)
    count_ref[...] = all_count_ref[pl.ds(pl.multiple_of(grp_ref[0] * OWN, OWN), OWN), :]


def output_target_kernel(grp_ref, got_ref, out_ref, keep_ref, send_ref, thin_ref, part_ref):
    for h in range(N_Z):
        thin_ref[:, h * HEAD_DIM : (h + 1) * HEAD_DIM] = got_ref[h, :, :HEAD_DIM].astype(F32)
    part_ref[...] = mm(thin_ref[...].astype(BF), out_ref[...])
    divide(grp_ref, part_ref, keep_ref, send_ref)


def slope_kernel(
    keep_ref, got_ref, keep_s_ref, got_s_ref, tokens_ref, seeds_ref, count_ref, out_ref, back_ref
):
    target_sum = keep_ref[...].astype(F32) + got_ref[...].astype(F32)
    student_sum = keep_s_ref[...].astype(F32) + got_s_ref[...].astype(F32)
    wanted = normalized(tokens_ref[...] + target_sum)[0].astype(BF).astype(F32)
    predicted, factor = normalized(seeds_ref[...] + student_sum)
    slope = jnp.clip(predicted - wanted, -1.0, 1.0) * count_ref[:, :1]
    back_ref[...] = (
        slope
        - jnp.mean(slope, axis=1, keepdims=True)
        - predicted * jnp.mean(slope * predicted, axis=1, keepdims=True)
    ) * factor
    columns = STRIPE * 2 * N_Z
    row = iota((columns, 2 * LANES), 0)
    col = iota((columns, 2 * LANES), 1)
    stripe = lax.div(col, 16)
    inner = lax.rem(col, 16)
    spread = jnp.where((inner < STRIPE) & (row == stripe * STRIPE + inner), 1.0, 0.0).astype(BF)
    for d in range(N_DP):
        part = back_ref[:, d * columns : (d + 1) * columns].astype(BF)
        part = mm(part, spread).astype(BF)
        out_ref[2 * d] = part
        out_ref[2 * d + 1] = part


def finish_kernel(core_ref, mine_ref, other_ref, out_ref):
    half = out_ref.shape[1] // 2
    total = jnp.zeros((out_ref.shape[0], 2 * WIDE), F32)
    for ref, flip in ((mine_ref, 0), (other_ref, 1)):
        side = core_ref[0] * (1 - 2 * flip) + flip
        row = iota((out_ref.shape[0], 16 * N_Z), 0)
        col = iota((out_ref.shape[0], 16 * N_Z), 1)
        stripe = side * N_Z + lax.div(col, 16)
        inner = lax.rem(col, 16)
        gather = jnp.where((inner < STRIPE) & (row == stripe * STRIPE + inner), 1.0, 0.0)
        total = total + mm(gather.astype(BF), ref[...])
    out_ref[:, :half] = total[:, :half]
    out_ref[:, half:] = total[:, WIDE : WIDE + half]


def blend_kernel(core_ref, target_ref, mine_ref, other_ref, out_ref):
    half = target_ref.shape[0] // 2
    left = jnp.where(core_ref[0] == 0, mine_ref[...], other_ref[...])
    right = jnp.where(core_ref[0] == 0, other_ref[...], mine_ref[...])
    for i, part in enumerate((left, right)):
        turned = jnp.transpose(part.astype(F32))[:half]
        rows = slice(i * half, (i + 1) * half)
        out_ref[rows, :] = MOMENTUM * target_ref[rows, :].astype(F32) + (1.0 - MOMENTUM) * turned


def ring(rows, gates):
    up = [(i, (i + 1) % N_Z) for i in range(N_Z)]
    down = [(i, (i - 1) % N_Z) for i in range(N_Z)]
    below = above = rows
    lower, upper = ([], [])
    for step in range(1, N_Z // 2):
        if step in gates:
            below, above, _ = lax.optimization_barrier((below, above, gates[step]))
        below = lax.ppermute(below, "z", up)
        above = lax.ppermute(above, "z", down)
        lower.append(below)
        upper.append(above)
    below = lax.ppermute(below, "z", up)
    return [rows] + lower + [below] + upper[::-1]


def body(
    clips, context, predict_index, target_qkv, target_out, student_qkv, student_out, mask_token
):
    tokens = clips[0]
    width = tokens.shape[1]
    half = width // 2
    z = lax.axis_index("z")
    core = lax.axis_index("core")
    grp = lax.axis_index("grp")
    z_at, core_at, grp_at = (v.astype(I32).reshape(1) for v in (z, core, grp))

    moved, perm = call(
        sorted_norm_kernel, (sds((BLOCK, width), BF), sds((BLOCK, BLOCK), BF))
    )(tokens, context)
    spacing = jnp.exp(jnp.arange(half, dtype=F32) * (-math.log(10000.0) / half))
    spot = jnp.arange(BLOCK, dtype=F32)
    t_angle = spot[:, None] * spacing[None, :]
    base = ((2 * jnp.arange(N_Z, dtype=I32) + core) * BLOCK).astype(F32)
    b_angle = base[:, None] * spacing[None, :]
    tables = (
        jnp.sin(t_angle),
        jnp.cos(t_angle),
        jnp.sin(b_angle),
        jnp.cos(b_angle),
    )
    table = pl.BlockSpec((BLOCK, half), lambda j: (0, 0))
    row = pl.BlockSpec((N_Z, half), lambda j: (0, 0))
    block = pl.BlockSpec((BLOCK, half), lambda j: (j, 0))
    seed_a, seed_b = call(
        seed_norm_kernel,
        (sds((N_Z * BLOCK, half), BF), sds((N_Z * BLOCK, half), BF)),
        grid=(N_Z,),
        in_specs=[table, table, row, row, pl.BlockSpec((2, half), lambda j: (0, 0))],
        out_specs=(block, block),
    )(
        *tables,
        mask_token.reshape(2, half),
    )
    listed = predict_index
    listed = jnp.concatenate([listed, lax.ppermute(listed, "core", SWAP)], axis=1)
    pieces = ring(moved, {2: (tables, listed), 3: (seed_a, seed_b)})

    head = call(
        head_kernel,
        sds((N_DP, width // N_DP, 2 * WIDE), BF),
        in_specs=[SMEM, SMEM] + [pl.BlockSpec()] * 3,
    )(z_at, core_at, after(target_qkv, moved), student_qkv, student_out.T)
    weights = after(exchange(head, DP), seed_a).reshape(width, 2 * WIDE)
    swapped = lax.ppermute(weights, "core", SWAP)

    rows_own = lax.dynamic_slice_in_dim(perm, CTX + grp * OWN, OWN, axis=0)
    tokens_own = mm(rows_own, tokens)
    places_own = jnp.sum(rows_own.astype(F32) * spot[None, :], axis=1)
    places_own = places_own + ((2 * z + core) * BLOCK).astype(F32)
    angle = places_own[:, None] * spacing[None, :]
    seeds = mask_token[None, :] + jnp.concatenate([jnp.sin(angle), jnp.cos(angle)], axis=1)

    head_w = pl.BlockSpec((width, WIDE), lambda i: (0, 0))
    out_w = pl.BlockSpec((width, WIDE), lambda i: (0, 1))
    query_t, kv, kvs = call(
        project_kernel,
        (
            sds((N_Z, TGT, LANES), BF),
            sds((N_Z * BLOCK, 2 * LANES), BF),
            sds((N_Z * CTX, 2 * LANES), BF),
        ),
        scratch=(
            pltpu.VMEM((N_Z * BLOCK, width), BF),
            pltpu.VMEM((N_Z * CTX, width), BF),
            pltpu.VMEM((width, WIDE), BF),
        ),
        grid=(1,),
        in_specs=[SMEM, SMEM] + [pl.BlockSpec()] * N_Z + [head_w] * 2,
    )(z_at, core_at, *pieces, weights, swapped)
    kvs_other = lax.ppermute(kvs, "core", SWAP)
    kv_other = lax.ppermute(kv, "core", SWAP)
    query_w = pl.BlockSpec((width, LANES), lambda j: (0, 0))
    query_s = call(
        seed_query_kernel,
        sds((N_Z * BLOCK, LANES), BF),
        grid=(N_Z // 2,),
        in_specs=[SMEM] + [pl.BlockSpec((2 * BLOCK, half), lambda j: (j, 0))] * 2 + [query_w] * 2,
        out_specs=pl.BlockSpec((2 * BLOCK, LANES), lambda j: (j, 0)),
    )(core_at, after(seed_a, kvs), seed_b, weights, swapped)

    mixed_s = call(
        attend_student_kernel, sds((N_Z, BLOCK, LANES), BF), in_specs=[SMEM] + [pl.BlockSpec()] * 4
    )(core_at, query_s, kvs, kvs_other, listed)
    mixed_s = exchange(mixed_s, "z")
    mixed_t = call(attend_target_kernel, sds((N_Z, TGT, LANES), BF))(query_t, kv, kv_other)
    mixed_t = exchange(after(mixed_t, mixed_s), "z")
    keep_s, send_s, mixed_c, count = call(
        output_student_kernel,
        (
            sds((OWN, width), BF),
            sds((OWN, width), BF),
            sds((N_DP, TGT, 2 * WIDE), BF),
            sds((OWN, LANES), F32),
        ),
        scratch=(
            pltpu.VMEM((BLOCK, N_Z * LANES), BF),
            pltpu.VMEM((TGT, 2 * WIDE), F32),
            pltpu.VMEM((TGT, width), F32),
            pltpu.VMEM((TGT, LANES), F32),
        ),
        grid=(1,),
        in_specs=[SMEM, SMEM] + [pl.BlockSpec()] * 2 + [out_w] * 2,
    )(grp_at, core_at, mixed_s, perm, weights, swapped)
    got_s = lax.ppermute(send_s, "grp", SWAP)
    keep, send = call(
        output_target_kernel,
        (sds((OWN, width), BF), sds((OWN, width), BF)),
        scratch=(pltpu.VMEM((TGT, N_Z * HEAD_DIM), F32), pltpu.VMEM((TGT, width), F32)),
        in_specs=[SMEM] + [pl.BlockSpec()] * 2,
    )(grp_at, after(mixed_t, got_s), target_out)
    got = lax.ppermute(send, "grp", SWAP)
    mixed_all = exchange(after(mixed_c, mixed_t), DP)
    mixed_all = mixed_all.reshape(N_DP * TGT, 2 * WIDE)
    stripes = call(
        slope_kernel, sds((2 * N_DP, OWN, 256), BF), scratch=(pltpu.VMEM((OWN, width), F32),)
    )(keep, got, keep_s, got_s, tokens_own, seeds, count)
    stripes = after(stripes, mixed_all)
    arrived = lax.all_to_all(stripes, (*DP, "grp"), split_axis=0, concat_axis=0, tiled=True)
    grad = lax.dot_general(
        arrived.reshape(N_DP * TGT, 256),
        mixed_all,
        (((0,), (0,)), ((), ())),
        preferred_element_type=F32,
    )
    lower, upper = (grad[: 16 * N_Z], grad[16 * N_Z :])
    grad_keep = jnp.where(core == 0, lower, upper)
    grad_send = jnp.where(core == 0, upper, lower)
    grad = grad_keep + lax.ppermute(grad_send, "core", SWAP)
    grad = grad.astype(BF).reshape(N_Z, 16, 2 * WIDE)
    pieces = exchange(grad, "z")
    turned = pl.BlockSpec((LANES, WIDE), lambda i: (i, 1))
    target_blend = call(
        blend_kernel,
        sds((half, width), F32),
        grid=(width // LANES,),
        in_specs=[SMEM, pl.BlockSpec((half, LANES), lambda i: (0, i)), turned, turned],
        out_specs=pl.BlockSpec((half, LANES), lambda i: (0, i)),
    )(core_at, after(target_out, grad), weights, swapped)
    grad = jnp.sum(pieces.astype(F32), axis=0).astype(BF)
    grad = to_all(after(grad, target_blend), "z", N_Z).reshape(16 * N_Z, 2 * WIDE)
    other = lax.ppermute(grad, "core", SWAP)
    out_grad = call(
        finish_kernel,
        sds((student_out.shape[1], student_out.shape[0]), F32),
        in_specs=[SMEM] + [pl.BlockSpec()] * 2,
    )(core_at, grad, other).T
    return (out_grad, target_blend)


def solution(mesh):
    fine = Mesh(mesh.devices.reshape(8, 2, 2, 2, 4), ("z", "core", "grp", "ylo", "x"))
    seq = ("z", "core")
    in_specs = (
        P(DP, seq, None),
        P(DP, seq),
        P(DP, seq),
        P(None, DP, "grp"),
        P("grp", None),
        P(None, DP, "grp"),
        P("grp", DP),
        P(),
    )
    out_specs = (P("grp", DP), P("grp", None))
    return jax.shard_map(body, mesh=fine, in_specs=in_specs, out_specs=out_specs, check_vma=False)
```

```python
import functools
import math

import jax
import jax.numpy as jnp
from jax import lax
from jax.experimental import pallas as pl
from jax.experimental.pallas import tpu as pltpu
from jax.sharding import Mesh, PartitionSpec as P


HEAD_DIM = 88
LANES = 128
WIDE = 384
CTX = 32
BLOCK = 128
TGT = 96
OWN = 48
N_Z = 8
N_DP = 8
STRIPE = 11
EPSILON = 1e-06
MOMENTUM = 0.99
SCALE = HEAD_DIM ** (-0.5)
BF = jnp.bfloat16
F32 = jnp.float32
I32 = jnp.int32
SWAP = [(0, 1), (1, 0)]
FLOPS = 10**6
DP = ("ylo", "x")
SMEM = pl.BlockSpec(memory_space=pltpu.SMEM)


def iota(shape, dim):
    return lax.broadcasted_iota(I32, shape, dim)


def mm(a, b):
    return jnp.dot(a, b, preferred_element_type=F32)


def mm_nt(a, b):
    return lax.dot_general(a, b, (((1,), (1,)), ((), ())), preferred_element_type=F32)


def sds(shape, dtype):
    return jax.ShapeDtypeStruct(shape, dtype)


def call(kernel, outs, scratch=(), flops=FLOPS, **specs):
    return pl.pallas_call(
        kernel,
        out_shape=outs,
        scratch_shapes=list(scratch),
        **specs,
        cost_estimate=pl.CostEstimate(flops=flops, bytes_accessed=10**6, transcendentals=0),
    )


def to_all(shard, axes, count):
    copies = jnp.broadcast_to(shard[None], (count, *shard.shape))
    return lax.all_to_all(copies, axes, split_axis=0, concat_axis=0, tiled=True)


def exchange(pieces, axes):
    return lax.all_to_all(pieces, axes, split_axis=0, concat_axis=0, tiled=True)


def after(value, others):
    return lax.optimization_barrier((value, others))[0]


def normalized(values):
    center = values - jnp.mean(values, axis=-1, keepdims=True)
    factor = lax.rsqrt(jnp.mean(center * center, axis=-1, keepdims=True) + EPSILON)
    return (center * factor, factor)


def sorted_norm_kernel(tokens_ref, context_ref, moved_ref, perm_ref):
    normed = normalized(tokens_ref[...].astype(F32))[0].astype(BF)
    flag = jnp.where(context_ref[...] == 1, 1.0, 0.0)
    upto = jnp.where(iota((BLOCK, BLOCK), 0) <= iota((BLOCK, BLOCK), 1), 1.0, 0.0).astype(BF)
    before = mm(jnp.broadcast_to(flag, (16, BLOCK)).astype(BF), upto)[:1]
    spot = iota((1, BLOCK), 1).astype(F32)
    rank = jnp.where(flag == 1.0, before - 1.0, CTX + spot - before).astype(I32)
    perm = jnp.where(rank == iota((BLOCK, BLOCK), 0), 1.0, 0.0).astype(BF)
    moved_ref[...] = mm(perm, normed).astype(BF)
    perm_ref[...] = perm


def head_kernel(z_ref, core_ref, target_ref, student_ref, turned_ref, head_ref, out_ref):
    rows = target_ref.shape[2]
    half = turned_ref.shape[1] // 2
    col = z_ref[0] * HEAD_DIM + iota((rows, LANES), 1)
    same = (iota((rows, LANES), 0) == col) & (iota((rows, LANES), 1) < HEAD_DIM)
    picked = jnp.where(same, 1.0, 0.0).astype(BF)

    def fill(ref, at):
        got = [mm(ref[k], picked).astype(BF) for k in range(3)]
        turned = turned_ref[:, at : at + half]
        rest = jnp.zeros((turned.shape[0], WIDE - half), BF)
        for d in range(N_DP):
            for k in range(3):
                head_ref[d, :, k * LANES : (k + 1) * LANES] = got[k]
            out_ref[d, :, :half] = turned
            out_ref[d, :, half:] = rest

    pl.when(core_ref[0] == 0)(lambda: fill(target_ref, 0))
    pl.when(core_ref[0] == 1)(lambda: fill(student_ref, half))


def seed_norm_kernel(sin_ref, cos_ref, bsin_ref, bcos_ref, mask_ref, lower_ref, upper_ref):
    half = sin_ref.shape[1]
    rows = 32
    bsin = bsin_ref[pl.ds(pl.program_id(0), 1), :]
    bcos = bcos_ref[pl.ds(pl.program_id(0), 1), :]

    def one(i, carry):
        at = pl.multiple_of(i * rows, rows)
        t_sin = sin_ref[pl.ds(at, rows), :]
        t_cos = cos_ref[pl.ds(at, rows), :]
        a = bsin * t_cos + bcos * t_sin + mask_ref[0:1, :]
        b = bcos * t_cos - bsin * t_sin + mask_ref[1:2, :]
        mean = (jnp.sum(a, -1, keepdims=True) + jnp.sum(b, -1, keepdims=True)) / (2 * half)
        a = a - mean
        b = b - mean
        var = (jnp.sum(a * a, -1, keepdims=True) + jnp.sum(b * b, -1, keepdims=True)) / (2 * half)
        inv = lax.rsqrt(var + EPSILON)
        lower_ref[pl.ds(at, rows), :] = (a * inv).astype(BF)
        upper_ref[pl.ds(at, rows), :] = (b * inv).astype(BF)
        return carry

    lax.fori_loop(0, BLOCK // rows, one, 0, unroll=2)


def seed_query_kernel(core_ref, lower_ref, upper_ref, mine_ref, other_ref, out_ref):
    half = lower_ref.shape[1]
    weight = jnp.where(core_ref[0] == 1, mine_ref[...], other_ref[...])
    query = mm(lower_ref[...], weight[:half]) + mm(upper_ref[...], weight[half:])
    out_ref[...] = query.astype(BF)


def project_kernel(z_ref, core_ref, *refs):
    pieces = refs[: N_Z - 1]
    mine_ref, other_ref, query_ref, kv_ref, kvs_ref, rows_ref, ctx_ref, target_ref = refs[N_Z - 1 :]
    slots = [d for d in range(N_Z) if d != N_Z // 2]
    for i in range(N_Z - 1):
        rows_ref[i * BLOCK : (i + 1) * BLOCK, :] = pieces[i][...]
        ctx_ref[i * CTX : (i + 1) * CTX, :] = pieces[i][:CTX, :]
    target_ref[...] = jnp.where(core_ref[0] == 0, mine_ref[...], other_ref[...])
    student = jnp.where(core_ref[0] == 0, other_ref[:, LANES:], mine_ref[:, LANES:])
    kvs_ref[...] = mm(ctx_ref[...], student).astype(BF)
    for at, count in ((0, 4), (4, 3)):
        rows = slice(at * BLOCK, (at + count) * BLOCK)
        got = mm(rows_ref[rows, :], target_ref[...]).astype(BF)
        kv_ref[rows, :] = got[:, LANES:]
        for k in range(count):
            dest = lax.rem(z_ref[0] - slots[at + k] + N_Z, N_Z)
            query_ref[dest] = got[k * BLOCK + CTX : (k + 1) * BLOCK, :LANES]


def project_last_kernel(
    z_ref, core_ref, last_ref, early_ref, kvs_early_ref, mine_ref, other_ref, query_ref, kv_ref, kvs_ref
):
    early = (N_Z - 1) * CTX
    target = jnp.where(core_ref[0] == 0, mine_ref[...], other_ref[...])
    student = jnp.where(core_ref[0] == 0, other_ref[:, LANES:], mine_ref[:, LANES:])
    kvs_ref[:early, :] = kvs_early_ref[...]
    kvs_ref[early:, :] = mm(last_ref[:CTX, :], student).astype(BF)
    got = mm(last_ref[...], target).astype(BF)
    kv_ref[...] = got[:, LANES:]
    query_ref[...] = early_ref[...]
    query_ref[lax.rem(z_ref[0] + N_Z // 2, N_Z)] = got[CTX:, :LANES]


def softmax_rows(query, pairs):
    scores = [mm_nt(query, pair[:, :LANES]) * SCALE for pair in pairs]
    peak = functools.reduce(jnp.maximum, [jnp.max(s, axis=1, keepdims=True) for s in scores])
    total, mixed = (0.0, 0.0)
    for s, pair in zip(scores, pairs):
        raised = jnp.exp(s - peak)
        total = total + jnp.sum(raised, axis=1, keepdims=True)
        mixed = mixed + mm(raised.astype(BF), pair[:, LANES:])
    return mixed / total


def attention_kernel(
    core_ref, query_ref, kv_ref, kv_other_ref, last_ref, last_other_ref, query_s_ref, kvs_ref,
    kvs_other_ref, listed_ref, out_ref,
):
    rows = 4 * TGT
    for i in range(2):
        query = query_ref[4 * i : 4 * i + 4].reshape(rows, LANES)
        mixed = softmax_rows(query, (kv_ref, kv_other_ref, last_ref, last_other_ref)).astype(BF)
        out_ref[4 * i : 4 * i + 4, :TGT, :] = mixed.reshape(4, TGT, LANES)
    rows = 4 * BLOCK
    lane = iota((rows, LANES), 1)
    slot = iota((rows, listed_ref.shape[1]), 0)
    for i in range(2):
        mixed = softmax_rows(query_s_ref[i * rows : (i + 1) * rows, :], (kvs_ref, kvs_other_ref))
        block = lax.div(slot, BLOCK)
        place = (2 * (4 * i + block) + core_ref[0]) * BLOCK + slot - block * BLOCK
        same = jnp.where(place == listed_ref[...], 1.0, 0.0)
        count = jnp.sum(same, axis=1, keepdims=True)
        mixed = jnp.where(lane == HEAD_DIM, count, mixed).astype(BF)
        out_ref[4 * i : 4 * i + 4, TGT:, :] = mixed.reshape(4, BLOCK, LANES)


def output_kernel(
    grp_ref, core_ref, got_ref, perm_ref, out_ref, mine_ref, other_ref, keep_ref, send_ref, mixed_ref,
    count_ref, wide_ref, thin_ref, thin_t_ref, part_ref, all_count_ref,
):
    for h in range(N_Z):
        wide_ref[:, h * LANES : (h + 1) * LANES] = got_ref[h, TGT:, :]
        thin_t_ref[:, h * HEAD_DIM : (h + 1) * HEAD_DIM] = got_ref[h, :TGT, :HEAD_DIM].astype(F32)
    chosen = mm(perm_ref[CTX:, :], wide_ref[...])
    lane = lax.rem(iota(chosen.shape, 1), LANES)
    all_count_ref[...] = jnp.broadcast_to(
        jnp.sum(jnp.where(lane == HEAD_DIM, chosen, 0.0), axis=1, keepdims=True), (TGT, LANES)
    )
    thin_ref[...] = jnp.zeros(thin_ref.shape, F32)
    for h in range(N_Z):
        at = (h // 4) * WIDE + (h % 4) * HEAD_DIM
        thin_ref[:, at : at + HEAD_DIM] = chosen[:, h * LANES : h * LANES + HEAD_DIM]
    mixed = thin_ref[...].astype(BF)
    for d in range(N_DP):
        mixed_ref[d] = mixed
    left = jnp.where(core_ref[0] == 0, mine_ref[...], other_ref[...])
    right = jnp.where(core_ref[0] == 0, other_ref[...], mine_ref[...])
    part_ref[:TGT, :] = mm(thin_t_ref[...].astype(BF), out_ref[...])
    part_ref[TGT:, :] = mm_nt(mixed[:, :WIDE], left) + mm_nt(mixed[:, WIDE:], right)
    mine = pl.multiple_of(grp_ref[0] * OWN, OWN)
    other = pl.multiple_of((1 - grp_ref[0]) * OWN, OWN)
    keep_ref[:OWN, :] = part_ref[pl.ds(mine, OWN), :].astype(BF)
    keep_ref[OWN:, :] = part_ref[pl.ds(TGT + mine, OWN), :].astype(BF)
    send_ref[:OWN, :] = part_ref[pl.ds(other, OWN), :].astype(BF)
    send_ref[OWN:, :] = part_ref[pl.ds(TGT + other, OWN), :].astype(BF)
    count_ref[...] = all_count_ref[pl.ds(mine, OWN), :]


def slope_kernel(
    keep_ref, got_ref, tokens_ref, seeds_ref, count_ref, out_ref, back_ref
):
    both = keep_ref[...].astype(F32) + got_ref[...].astype(F32)
    wanted = normalized(tokens_ref[...] + both[:OWN])[0].astype(BF).astype(F32)
    predicted, factor = normalized(seeds_ref[...] + both[OWN:])
    slope = jnp.clip(predicted - wanted, -1.0, 1.0) * count_ref[:, :1]
    back_ref[...] = (
        slope
        - jnp.mean(slope, axis=1, keepdims=True)
        - predicted * jnp.mean(slope * predicted, axis=1, keepdims=True)
    ) * factor
    columns = STRIPE * 2 * N_Z
    row = iota((columns, 2 * LANES), 0)
    col = iota((columns, 2 * LANES), 1)
    stripe = lax.div(col, 16)
    inner = lax.rem(col, 16)
    spread = jnp.where((inner < STRIPE) & (row == stripe * STRIPE + inner), 1.0, 0.0).astype(BF)
    for d in range(N_DP):
        part = back_ref[:, d * columns : (d + 1) * columns].astype(BF)
        part = mm(part, spread).astype(BF)
        out_ref[2 * d] = part
        out_ref[2 * d + 1] = part


def finish_kernel(core_ref, mine_ref, other_ref, out_ref):
    half = out_ref.shape[1] // 2
    total = jnp.zeros((out_ref.shape[0], 2 * WIDE), F32)
    for ref, flip in ((mine_ref, 0), (other_ref, 1)):
        side = core_ref[0] * (1 - 2 * flip) + flip
        row = iota((out_ref.shape[0], 16 * N_Z), 0)
        col = iota((out_ref.shape[0], 16 * N_Z), 1)
        stripe = side * N_Z + lax.div(col, 16)
        inner = lax.rem(col, 16)
        gather = jnp.where((inner < STRIPE) & (row == stripe * STRIPE + inner), 1.0, 0.0)
        total = total + mm(gather.astype(BF), ref[...])
    out_ref[:, :half] = total[:, :half]
    out_ref[:, half:] = total[:, WIDE : WIDE + half]


def blend_kernel(core_ref, target_ref, mine_ref, other_ref, out_ref):
    half = target_ref.shape[0] // 2
    left = jnp.where(core_ref[0] == 0, mine_ref[...], other_ref[...])
    right = jnp.where(core_ref[0] == 0, other_ref[...], mine_ref[...])
    for i, part in enumerate((left, right)):
        turned = jnp.transpose(part.astype(F32))[:half]
        rows = slice(i * half, (i + 1) * half)
        out_ref[rows, :] = MOMENTUM * target_ref[rows, :].astype(F32) + (1.0 - MOMENTUM) * turned


def ring(rows, gates):
    up = [(i, (i + 1) % N_Z) for i in range(N_Z)]
    down = [(i, (i - 1) % N_Z) for i in range(N_Z)]
    below = above = rows
    lower, upper = ([], [])
    for step in range(1, N_Z // 2):
        if step in gates:
            below, above, _ = lax.optimization_barrier((below, above, gates[step]))
        below = lax.ppermute(below, "z", up)
        above = lax.ppermute(above, "z", down)
        lower.append(below)
        upper.append(above)
    below = lax.ppermute(below, "z", up)
    return [rows] + lower + [below] + upper[::-1]


def body(
    clips, context, predict_index, target_qkv, target_out, student_qkv, student_out, mask_token
):
    tokens = clips[0]
    width = tokens.shape[1]
    half = width // 2
    z = lax.axis_index("z")
    core = lax.axis_index("core")
    grp = lax.axis_index("grp")
    z_at, core_at, grp_at = (v.astype(I32).reshape(1) for v in (z, core, grp))

    moved, perm = call(
        sorted_norm_kernel, (sds((BLOCK, width), BF), sds((BLOCK, BLOCK), BF))
    )(tokens, context)
    spacing = jnp.exp(jnp.arange(half, dtype=F32) * (-math.log(10000.0) / half))
    spot = jnp.arange(BLOCK, dtype=F32)
    t_angle = spot[:, None] * spacing[None, :]
    base = ((2 * jnp.arange(N_Z, dtype=I32) + core) * BLOCK).astype(F32)
    b_angle = base[:, None] * spacing[None, :]
    tables = (
        jnp.sin(t_angle),
        jnp.cos(t_angle),
        jnp.sin(b_angle),
        jnp.cos(b_angle),
    )
    table = pl.BlockSpec((BLOCK, half), lambda j: (0, 0))
    row = pl.BlockSpec((N_Z, half), lambda j: (0, 0))
    block = pl.BlockSpec((BLOCK, half), lambda j: (j, 0))
    seed_a, seed_b = call(
        seed_norm_kernel,
        (sds((N_Z * BLOCK, half), BF), sds((N_Z * BLOCK, half), BF)),
        grid=(N_Z,),
        in_specs=[table, table, row, row, pl.BlockSpec((2, half), lambda j: (0, 0))],
        out_specs=(block, block),
    )(
        *tables,
        mask_token.reshape(2, half),
    )
    listed = predict_index
    listed = jnp.concatenate([listed, lax.ppermute(listed, "core", SWAP)], axis=1)
    pieces = ring(moved, {2: (tables, listed), 3: (seed_a, seed_b)})

    piece = sds((N_DP, width // N_DP, WIDE), BF)
    head, turned = call(
        head_kernel, (piece, piece), in_specs=[SMEM, SMEM] + [pl.BlockSpec()] * 3
    )(z_at, core_at, after(target_qkv, moved), student_qkv, student_out.T)
    weights = exchange(head, DP)
    weights = after(weights, seed_a).reshape(width, WIDE)
    swapped = lax.ppermute(weights, "core", SWAP)
    out_mine = exchange(after(turned, weights), DP).reshape(width, WIDE)
    out_other = lax.ppermute(out_mine, "core", SWAP)

    rows_own = lax.dynamic_slice_in_dim(perm, CTX + grp * OWN, OWN, axis=0)
    tokens_own = mm(rows_own, tokens)
    places_own = jnp.sum(rows_own.astype(F32) * spot[None, :], axis=1)
    places_own = places_own + ((2 * z + core) * BLOCK).astype(F32)
    angle = places_own[:, None] * spacing[None, :]
    seeds = mask_token[None, :] + jnp.concatenate([jnp.sin(angle), jnp.cos(angle)], axis=1)

    query_w = pl.BlockSpec((width, LANES), lambda j: (0, 0))
    query_s = call(
        seed_query_kernel,
        sds((N_Z * BLOCK, LANES), BF),
        grid=(N_Z // 2,),
        in_specs=[SMEM] + [pl.BlockSpec((2 * BLOCK, half), lambda j: (j, 0))] * 2 + [query_w] * 2,
        out_specs=pl.BlockSpec((2 * BLOCK, LANES), lambda j: (j, 0)),
    )(core_at, seed_a, seed_b, weights, swapped)
    early = pieces[: N_Z // 2] + pieces[N_Z // 2 + 1 :]
    query_t, kv, kvs = call(
        project_kernel,
        (
            sds((N_Z, TGT, LANES), BF),
            sds(((N_Z - 1) * BLOCK, 2 * LANES), BF),
            sds(((N_Z - 1) * CTX, 2 * LANES), BF),
        ),
        scratch=(
            pltpu.VMEM(((N_Z - 1) * BLOCK, width), BF),
            pltpu.VMEM(((N_Z - 1) * CTX, width), BF),
            pltpu.VMEM((width, WIDE), BF),
        ),
        in_specs=[SMEM, SMEM] + [pl.BlockSpec()] * (N_Z + 1),
    )(z_at, core_at, *early, after(weights, query_s), swapped)
    kv_other = lax.ppermute(kv, "core", SWAP)
    query_t, kv_last, kvs = call(
        project_last_kernel,
        (
            sds((N_Z, TGT, LANES), BF),
            sds((BLOCK, 2 * LANES), BF),
            sds((N_Z * CTX, 2 * LANES), BF),
        ),
        in_specs=[SMEM, SMEM] + [pl.BlockSpec()] * 5,
    )(z_at, core_at, pieces[N_Z // 2], query_t, kvs, weights, swapped)
    kvs_other = lax.ppermute(kvs, "core", SWAP)
    last_other = lax.ppermute(kv_last, "core", SWAP)
    mixed = call(
        attention_kernel, sds((N_Z, TGT + BLOCK, LANES), BF), in_specs=[SMEM] + [pl.BlockSpec()] * 9
    )(core_at, query_t, kv, kv_other, kv_last, last_other, query_s, kvs, kvs_other, listed)
    mixed = exchange(after(mixed, out_mine), "z")
    keep, send, mixed_c, count = call(
        output_kernel,
        (
            sds((2 * OWN, width), BF),
            sds((2 * OWN, width), BF),
            sds((N_DP, TGT, 2 * WIDE), BF),
            sds((OWN, LANES), F32),
        ),
        scratch=(
            pltpu.VMEM((BLOCK, N_Z * LANES), BF),
            pltpu.VMEM((TGT, 2 * WIDE), F32),
            pltpu.VMEM((TGT, N_Z * HEAD_DIM), F32),
            pltpu.VMEM((2 * TGT, width), F32),
            pltpu.VMEM((TGT, LANES), F32),
        ),
        in_specs=[SMEM, SMEM] + [pl.BlockSpec()] * 5,
    )(grp_at, core_at, mixed, perm, target_out, out_mine, out_other)
    got = lax.ppermute(send, "grp", SWAP)
    mixed_all = exchange(mixed_c, DP)
    mixed_all = mixed_all.reshape(N_DP * TGT, 2 * WIDE)
    stripes = call(
        slope_kernel, sds((2 * N_DP, OWN, 256), BF), scratch=(pltpu.VMEM((OWN, width), F32),)
    )(keep, got, tokens_own, seeds, count)
    stripes = after(stripes, mixed_all)
    arrived = lax.all_to_all(stripes, (*DP, "grp"), split_axis=0, concat_axis=0, tiled=True)
    grad = lax.dot_general(
        arrived.reshape(N_DP * TGT, 256),
        mixed_all,
        (((0,), (0,)), ((), ())),
        preferred_element_type=F32,
    )
    lower, upper = (grad[: 16 * N_Z], grad[16 * N_Z :])
    grad_keep = jnp.where(core == 0, lower, upper)
    grad_send = jnp.where(core == 0, upper, lower)
    grad = grad_keep + lax.ppermute(grad_send, "core", SWAP)
    grad = grad.astype(BF).reshape(N_Z, 16, 2 * WIDE)
    pieces = exchange(grad, "z")
    turned = pl.BlockSpec((LANES, WIDE), lambda i: (i, 0))
    target_blend = call(
        blend_kernel,
        sds((half, width), F32),
        grid=(width // LANES,),
        in_specs=[SMEM, pl.BlockSpec((half, LANES), lambda i: (0, i)), turned, turned],
        out_specs=pl.BlockSpec((half, LANES), lambda i: (0, i)),
    )(core_at, after(target_out, grad), out_mine, out_other)
    grad = jnp.sum(pieces.astype(F32), axis=0).astype(BF)
    grad = to_all(after(grad, target_blend), "z", N_Z).reshape(16 * N_Z, 2 * WIDE)
    other = lax.ppermute(grad, "core", SWAP)
    out_grad = call(
        finish_kernel,
        sds((student_out.shape[1], student_out.shape[0]), F32),
        in_specs=[SMEM] + [pl.BlockSpec()] * 2,
    )(core_at, grad, other).T
    return (out_grad, target_blend)


def solution(mesh):
    fine = Mesh(mesh.devices.reshape(8, 2, 2, 2, 4), ("z", "core", "grp", "ylo", "x"))
    seq = ("z", "core")
    in_specs = (
        P(DP, seq, None),
        P(DP, seq),
        P(DP, seq),
        P(None, DP, "grp"),
        P("grp", None),
        P(None, DP, "grp"),
        P("grp", DP),
        P(),
    )
    out_specs = (P("grp", DP), P("grp", None))
    return jax.shard_map(body, mesh=fine, in_specs=in_specs, out_specs=out_specs, check_vma=False)
```

```python
import functools
import math

import jax
import jax.numpy as jnp
from jax import lax
from jax.experimental import pallas as pl
from jax.experimental.pallas import tpu as pltpu
from jax.sharding import Mesh, PartitionSpec as P


HEAD_DIM = 88
LANES = 128
WIDE = 384
CTX = 32
BLOCK = 128
TGT = 96
OWN = 48
N_Z = 8
N_DP = 8
STRIPE = 11
EPSILON = 1e-06
MOMENTUM = 0.99
SCALE = HEAD_DIM ** (-0.5)
BF = jnp.bfloat16
F32 = jnp.float32
I32 = jnp.int32
SWAP = [(0, 1), (1, 0)]
FLOPS = 10**6
DP = ("ylo", "x")
SMEM = pl.BlockSpec(memory_space=pltpu.SMEM)


def iota(shape, dim):
    return lax.broadcasted_iota(I32, shape, dim)


def mm(a, b):
    return jnp.dot(a, b, preferred_element_type=F32)


def mm_nt(a, b):
    return lax.dot_general(a, b, (((1,), (1,)), ((), ())), preferred_element_type=F32)


def sds(shape, dtype):
    return jax.ShapeDtypeStruct(shape, dtype)


def call(kernel, outs, scratch=(), flops=FLOPS, **specs):
    return pl.pallas_call(
        kernel,
        out_shape=outs,
        scratch_shapes=list(scratch),
        **specs,
        cost_estimate=pl.CostEstimate(flops=flops, bytes_accessed=10**6, transcendentals=0),
    )


def to_all(shard, axes, count):
    copies = jnp.broadcast_to(shard[None], (count, *shard.shape))
    return lax.all_to_all(copies, axes, split_axis=0, concat_axis=0, tiled=True)


def exchange(pieces, axes):
    return lax.all_to_all(pieces, axes, split_axis=0, concat_axis=0, tiled=True)


def on_chip(value):
    return pltpu.with_memory_space_constraint(value, pltpu.VMEM)


def after(value, others):
    return lax.optimization_barrier((value, others))[0]


def normalized(values):
    center = values - jnp.mean(values, axis=-1, keepdims=True)
    factor = lax.rsqrt(jnp.mean(center * center, axis=-1, keepdims=True) + EPSILON)
    return (center * factor, factor)


def sorted_norm_kernel(tokens_ref, context_ref, moved_ref, perm_ref):
    normed = normalized(tokens_ref[...].astype(F32))[0].astype(BF)
    flag = jnp.where(context_ref[...] == 1, 1.0, 0.0)
    upto = jnp.where(iota((BLOCK, BLOCK), 0) <= iota((BLOCK, BLOCK), 1), 1.0, 0.0).astype(BF)
    before = mm(jnp.broadcast_to(flag, (16, BLOCK)).astype(BF), upto)[:1]
    spot = iota((1, BLOCK), 1).astype(F32)
    rank = jnp.where(flag == 1.0, before - 1.0, CTX + spot - before).astype(I32)
    perm = jnp.where(rank == iota((BLOCK, BLOCK), 0), 1.0, 0.0).astype(BF)
    moved_ref[...] = mm(perm, normed).astype(BF)
    perm_ref[...] = perm


def head_kernel(z_ref, core_ref, target_ref, student_ref, turned_ref, head_ref, out_ref):
    rows = target_ref.shape[2]
    half = turned_ref.shape[1] // 2
    col = z_ref[0] * HEAD_DIM + iota((rows, LANES), 1)
    same = (iota((rows, LANES), 0) == col) & (iota((rows, LANES), 1) < HEAD_DIM)
    picked = jnp.where(same, 1.0, 0.0).astype(BF)

    def fill(ref, at):
        got = [mm(ref[k], picked).astype(BF) for k in range(3)]
        turned = turned_ref[:, at : at + half]
        rest = jnp.zeros((turned.shape[0], WIDE - half), BF)
        for d in range(N_DP):
            for k in range(3):
                head_ref[d, :, k * LANES : (k + 1) * LANES] = got[k]
            out_ref[d, :, :half] = turned
            out_ref[d, :, half:] = rest

    pl.when(core_ref[0] == 0)(lambda: fill(target_ref, 0))
    pl.when(core_ref[0] == 1)(lambda: fill(student_ref, half))


def seed_norm_kernel(sin_ref, cos_ref, mask_ref, lower_ref, upper_ref, t_sin_ref, t_cos_ref):
    half = sin_ref.shape[1]
    width = 2 * half
    fine = N_Z
    coarse = BLOCK // N_Z

    def rows_of(at, count):
        return (sin_ref[pl.ds(at, count), :], cos_ref[pl.ds(at, count), :])

    @pl.when(pl.program_id(0) == 0)
    def tables():
        small_sin, small_cos = rows_of(N_Z, fine)
        for i in range(coarse):
            big_sin, big_cos = rows_of(N_Z + fine + i, 1)
            t_sin_ref[i * fine : (i + 1) * fine, :] = big_sin * small_cos + big_cos * small_sin
            t_cos_ref[i * fine : (i + 1) * fine, :] = big_cos * small_cos - big_sin * small_sin

    b_sin, b_cos = rows_of(pl.program_id(0), 1)
    mask = mask_ref[...] - jnp.mean(mask_ref[...])
    mask_a = mask[:, :half]
    mask_b = mask[:, half:]
    rows = 32
    for i in range(BLOCK // rows):
        part = slice(i * rows, (i + 1) * rows)
        t_sin = t_sin_ref[part, :]
        t_cos = t_cos_ref[part, :]
        a = b_sin * t_cos + b_cos * t_sin + mask_a
        b = b_cos * t_cos - b_sin * t_sin + mask_b
        mean = (jnp.sum(a, -1, keepdims=True) + jnp.sum(b, -1, keepdims=True)) / width
        square = (jnp.sum(a * a, -1, keepdims=True) + jnp.sum(b * b, -1, keepdims=True)) / width
        inv = lax.rsqrt(jnp.maximum(square - mean * mean, 0.0) + EPSILON)
        lower_ref[part, :] = ((a - mean) * inv).astype(BF)
        upper_ref[part, :] = ((b - mean) * inv).astype(BF)


def seed_query_kernel(core_ref, lower_ref, upper_ref, mine_ref, other_ref, out_ref):
    half = lower_ref.shape[1]
    weight = jnp.where(core_ref[0] == 1, mine_ref[...], other_ref[...])
    query = mm(lower_ref[...], weight[:half]) + mm(upper_ref[...], weight[half:])
    out_ref[...] = query.astype(BF)


def project_kernel(z_ref, core_ref, *refs):
    pieces = refs[: N_Z - 1]
    mine_ref, other_ref, query_ref, kv_ref, kvs_ref, rows_ref, ctx_ref, target_ref = refs[N_Z - 1 :]
    slots = [d for d in range(N_Z) if d != N_Z // 2]
    for i in range(N_Z - 1):
        rows_ref[i * BLOCK : (i + 1) * BLOCK, :] = pieces[i][...]
        ctx_ref[i * CTX : (i + 1) * CTX, :] = pieces[i][:CTX, :]
    target_ref[...] = jnp.where(core_ref[0] == 0, mine_ref[...], other_ref[...])
    student = jnp.where(core_ref[0] == 0, other_ref[:, LANES:], mine_ref[:, LANES:])
    kvs_ref[...] = mm(ctx_ref[...], student).astype(BF)
    for at, count in ((0, 4), (4, 3)):
        rows = slice(at * BLOCK, (at + count) * BLOCK)
        got = mm(rows_ref[rows, :], target_ref[...]).astype(BF)
        kv_ref[rows, :] = got[:, LANES:]
        for k in range(count):
            dest = lax.rem(z_ref[0] - slots[at + k] + N_Z, N_Z)
            query_ref[dest] = got[k * BLOCK + CTX : (k + 1) * BLOCK, :LANES]


def project_last_kernel(
    z_ref, core_ref, last_ref, early_ref, kvs_early_ref, mine_ref, other_ref, query_ref, kv_ref, kvs_ref
):
    early = (N_Z - 1) * CTX
    target = jnp.where(core_ref[0] == 0, mine_ref[...], other_ref[...])
    student = jnp.where(core_ref[0] == 0, other_ref[:, LANES:], mine_ref[:, LANES:])
    kvs_ref[:early, :] = kvs_early_ref[...]
    kvs_ref[early:, :] = mm(last_ref[:CTX, :], student).astype(BF)
    got = mm(last_ref[...], target).astype(BF)
    kv_ref[...] = got[:, LANES:]
    query_ref[...] = early_ref[...]
    query_ref[lax.rem(z_ref[0] + N_Z // 2, N_Z)] = got[CTX:, :LANES]


def softmax_rows(query, pairs):
    scores = [mm_nt(query, pair[:, :LANES]) * SCALE for pair in pairs]
    peak = functools.reduce(jnp.maximum, [jnp.max(s, axis=1, keepdims=True) for s in scores])
    total, mixed = (0.0, 0.0)
    for s, pair in zip(scores, pairs):
        raised = jnp.exp(s - peak)
        total = total + jnp.sum(raised, axis=1, keepdims=True)
        mixed = mixed + mm(raised.astype(BF), pair[:, LANES:])
    return mixed / total


def attention_kernel(
    core_ref, query_ref, kv_ref, kv_other_ref, last_ref, last_other_ref, query_s_ref, kvs_ref,
    kvs_other_ref, listed_ref, out_ref,
):
    rows = 4 * TGT
    for i in range(2):
        query = query_ref[4 * i : 4 * i + 4].reshape(rows, LANES)
        mixed = softmax_rows(query, (kv_ref, kv_other_ref, last_ref, last_other_ref)).astype(BF)
        out_ref[4 * i : 4 * i + 4, :TGT, :] = mixed.reshape(4, TGT, LANES)
    rows = 4 * BLOCK
    lane = iota((rows, LANES), 1)
    slot = iota((rows, listed_ref.shape[1]), 0)
    for i in range(2):
        mixed = softmax_rows(query_s_ref[i * rows : (i + 1) * rows, :], (kvs_ref, kvs_other_ref))
        block = lax.div(slot, BLOCK)
        place = (2 * (4 * i + block) + core_ref[0]) * BLOCK + slot - block * BLOCK
        same = jnp.where(place == listed_ref[...], 1.0, 0.0)
        count = jnp.sum(same, axis=1, keepdims=True)
        mixed = jnp.where(lane == HEAD_DIM, count, mixed).astype(BF)
        out_ref[4 * i : 4 * i + 4, TGT:, :] = mixed.reshape(4, BLOCK, LANES)


def output_kernel(
    grp_ref, core_ref, got_ref, perm_ref, out_ref, mine_ref, other_ref, keep_ref, send_ref, mixed_ref,
    count_ref, wide_ref, thin_ref, thin_t_ref, part_ref, all_count_ref,
):
    for h in range(N_Z):
        wide_ref[:, h * LANES : (h + 1) * LANES] = got_ref[h, TGT:, :]
        thin_t_ref[:, h * HEAD_DIM : (h + 1) * HEAD_DIM] = got_ref[h, :TGT, :HEAD_DIM].astype(F32)
    chosen = mm(perm_ref[CTX:, :], wide_ref[...])
    lane = lax.rem(iota(chosen.shape, 1), LANES)
    all_count_ref[...] = jnp.broadcast_to(
        jnp.sum(jnp.where(lane == HEAD_DIM, chosen, 0.0), axis=1, keepdims=True), (TGT, LANES)
    )
    thin_ref[...] = jnp.zeros(thin_ref.shape, F32)
    for h in range(N_Z):
        at = (h // 4) * WIDE + (h % 4) * HEAD_DIM
        thin_ref[:, at : at + HEAD_DIM] = chosen[:, h * LANES : h * LANES + HEAD_DIM]
    mixed = thin_ref[...].astype(BF)
    for d in range(N_DP):
        mixed_ref[d] = mixed
    left = jnp.where(core_ref[0] == 0, mine_ref[...], other_ref[...])
    right = jnp.where(core_ref[0] == 0, other_ref[...], mine_ref[...])
    part_ref[:TGT, :] = mm(thin_t_ref[...].astype(BF), out_ref[...])
    part_ref[TGT:, :] = mm_nt(mixed[:, :WIDE], left) + mm_nt(mixed[:, WIDE:], right)
    mine = pl.multiple_of(grp_ref[0] * OWN, OWN)
    other = pl.multiple_of((1 - grp_ref[0]) * OWN, OWN)
    keep_ref[:OWN, :] = part_ref[pl.ds(mine, OWN), :].astype(BF)
    keep_ref[OWN:, :] = part_ref[pl.ds(TGT + mine, OWN), :].astype(BF)
    send_ref[:OWN, :] = part_ref[pl.ds(other, OWN), :].astype(BF)
    send_ref[OWN:, :] = part_ref[pl.ds(TGT + other, OWN), :].astype(BF)
    count_ref[...] = all_count_ref[pl.ds(mine, OWN), :]


def slope_kernel(
    keep_ref, got_ref, tokens_ref, seeds_ref, count_ref, out_ref, back_ref
):
    both = keep_ref[...].astype(F32) + got_ref[...].astype(F32)
    wanted = normalized(tokens_ref[...] + both[:OWN])[0].astype(BF).astype(F32)
    predicted, factor = normalized(seeds_ref[...] + both[OWN:])
    slope = jnp.clip(predicted - wanted, -1.0, 1.0) * count_ref[:, :1]
    back_ref[...] = (
        slope
        - jnp.mean(slope, axis=1, keepdims=True)
        - predicted * jnp.mean(slope * predicted, axis=1, keepdims=True)
    ) * factor
    columns = STRIPE * 2 * N_Z
    row = iota((columns, 2 * LANES), 0)
    col = iota((columns, 2 * LANES), 1)
    stripe = lax.div(col, 16)
    inner = lax.rem(col, 16)
    spread = jnp.where((inner < STRIPE) & (row == stripe * STRIPE + inner), 1.0, 0.0).astype(BF)
    for d in range(N_DP):
        part = back_ref[:, d * columns : (d + 1) * columns].astype(BF)
        part = mm(part, spread).astype(BF)
        out_ref[2 * d] = part
        out_ref[2 * d + 1] = part


def finish_kernel(core_ref, mine_ref, other_ref, out_ref):
    half = out_ref.shape[1] // 2
    total = jnp.zeros((out_ref.shape[0], 2 * WIDE), F32)
    for ref, flip in ((mine_ref, 0), (other_ref, 1)):
        side = core_ref[0] * (1 - 2 * flip) + flip
        row = iota((out_ref.shape[0], 16 * N_Z), 0)
        col = iota((out_ref.shape[0], 16 * N_Z), 1)
        stripe = side * N_Z + lax.div(col, 16)
        inner = lax.rem(col, 16)
        gather = jnp.where((inner < STRIPE) & (row == stripe * STRIPE + inner), 1.0, 0.0)
        total = total + mm(gather.astype(BF), ref[...])
    out_ref[:, :half] = total[:, :half]
    out_ref[:, half:] = total[:, WIDE : WIDE + half]


def blend_kernel(core_ref, target_ref, mine_ref, other_ref, out_ref):
    half = target_ref.shape[0] // 2
    left = jnp.where(core_ref[0] == 0, mine_ref[...], other_ref[...])
    right = jnp.where(core_ref[0] == 0, other_ref[...], mine_ref[...])
    for i, part in enumerate((left, right)):
        turned = jnp.transpose(part.astype(F32))[:half]
        rows = slice(i * half, (i + 1) * half)
        out_ref[rows, :] = MOMENTUM * target_ref[rows, :].astype(F32) + (1.0 - MOMENTUM) * turned


def ring(rows, gates):
    up = [(i, (i + 1) % N_Z) for i in range(N_Z)]
    down = [(i, (i - 1) % N_Z) for i in range(N_Z)]
    below = above = rows
    lower, upper = ([], [])
    for step in range(1, N_Z // 2):
        if step in gates:
            below, above, _ = lax.optimization_barrier((below, above, gates[step]))
        below = lax.ppermute(below, "z", up)
        above = lax.ppermute(above, "z", down)
        lower.append(below)
        upper.append(above)
    below = lax.ppermute(below, "z", up)
    return [rows] + lower + [below] + upper[::-1]


def body(
    clips, context, predict_index, target_qkv, target_out, student_qkv, student_out, mask_token
):
    tokens = clips[0]
    width = tokens.shape[1]
    half = width // 2
    z = lax.axis_index("z")
    core = lax.axis_index("core")
    grp = lax.axis_index("grp")
    z_at, core_at, grp_at = (v.astype(I32).reshape(1) for v in (z, core, grp))

    moved, perm = call(
        sorted_norm_kernel, (sds((BLOCK, width), BF), sds((BLOCK, BLOCK), BF))
    )(tokens, context)
    spacing = jnp.exp(jnp.arange(half, dtype=F32) * (-math.log(10000.0) / half))
    spot = jnp.arange(BLOCK, dtype=F32)
    base = (2 * jnp.arange(N_Z, dtype=I32) + core) * BLOCK
    steps = jnp.concatenate(
        [base, jnp.arange(N_Z, dtype=I32), N_Z * jnp.arange(BLOCK // N_Z, dtype=I32)]
    )
    angles = steps.astype(F32)[:, None] * spacing[None, :]
    tables = (jnp.sin(angles), jnp.cos(angles))
    block = pl.BlockSpec((BLOCK, half), lambda j: (j, 0))
    seed_a, seed_b = call(
        seed_norm_kernel,
        (sds((N_Z * BLOCK, half), BF), sds((N_Z * BLOCK, half), BF)),
        scratch=(pltpu.VMEM((BLOCK, half), F32), pltpu.VMEM((BLOCK, half), F32)),
        grid=(N_Z,),
        in_specs=[pl.BlockSpec(angles.shape, lambda j: (0, 0))] * 2
        + [pl.BlockSpec((1, width), lambda j: (0, 0))],
        out_specs=(block, block),
    )(*tables, mask_token[None])
    listed = predict_index
    listed = jnp.concatenate([listed, lax.ppermute(listed, "core", SWAP)], axis=1)
    pieces = ring(moved, {2: (tables, listed), 3: (seed_a, seed_b)})

    piece = sds((N_DP, width // N_DP, WIDE), BF)
    head, turned = call(
        head_kernel, (piece, piece), in_specs=[SMEM, SMEM] + [pl.BlockSpec()] * 3
    )(z_at, core_at, after(target_qkv, moved), student_qkv, student_out.T)
    weights = exchange(head, DP)
    weights = after(weights, seed_a).reshape(width, WIDE)
    swapped = lax.ppermute(weights, "core", SWAP)
    out_mine = exchange(after(turned, weights), DP).reshape(width, WIDE)
    out_other = lax.ppermute(out_mine, "core", SWAP)

    rows_own = lax.dynamic_slice_in_dim(perm, CTX + grp * OWN, OWN, axis=0)
    tokens_own = mm(rows_own, tokens)
    places_own = jnp.sum(rows_own.astype(F32) * spot[None, :], axis=1)
    places_own = places_own + ((2 * z + core) * BLOCK).astype(F32)
    angle = places_own[:, None] * spacing[None, :]
    seeds = mask_token[None, :] + jnp.concatenate([jnp.sin(angle), jnp.cos(angle)], axis=1)

    query_w = pl.BlockSpec((width, LANES), lambda j: (0, 0))
    query_s = call(
        seed_query_kernel,
        sds((N_Z * BLOCK, LANES), BF),
        grid=(N_Z // 2,),
        in_specs=[SMEM] + [pl.BlockSpec((2 * BLOCK, half), lambda j: (j, 0))] * 2 + [query_w] * 2,
        out_specs=pl.BlockSpec((2 * BLOCK, LANES), lambda j: (j, 0)),
    )(core_at, seed_a, seed_b, weights, swapped)
    early = pieces[: N_Z // 2] + pieces[N_Z // 2 + 1 :]
    query_t, kv, kvs = call(
        project_kernel,
        (
            sds((N_Z, TGT, LANES), BF),
            sds(((N_Z - 1) * BLOCK, 2 * LANES), BF),
            sds(((N_Z - 1) * CTX, 2 * LANES), BF),
        ),
        scratch=(
            pltpu.VMEM(((N_Z - 1) * BLOCK, width), BF),
            pltpu.VMEM(((N_Z - 1) * CTX, width), BF),
            pltpu.VMEM((width, WIDE), BF),
        ),
        in_specs=[SMEM, SMEM] + [pl.BlockSpec()] * (N_Z + 1),
    )(z_at, core_at, *early, after(weights, query_s), swapped)
    kv_other = lax.ppermute(kv, "core", SWAP)
    query_t, kv_last, kvs = call(
        project_last_kernel,
        (
            sds((N_Z, TGT, LANES), BF),
            sds((BLOCK, 2 * LANES), BF),
            sds((N_Z * CTX, 2 * LANES), BF),
        ),
        in_specs=[SMEM, SMEM] + [pl.BlockSpec()] * 5,
    )(z_at, core_at, on_chip(pieces[N_Z // 2]), query_t, kvs, weights, swapped)
    kvs_other = lax.ppermute(kvs, "core", SWAP)
    last_other = lax.ppermute(kv_last, "core", SWAP)
    mixed = call(
        attention_kernel, sds((N_Z, TGT + BLOCK, LANES), BF), in_specs=[SMEM] + [pl.BlockSpec()] * 9
    )(
        core_at,
        query_t,
        kv,
        on_chip(kv_other),
        kv_last,
        on_chip(last_other),
        query_s,
        kvs,
        on_chip(kvs_other),
        listed,
    )
    mixed = exchange(after(mixed, out_mine), "z")
    keep, send, mixed_c, count = call(
        output_kernel,
        (
            sds((2 * OWN, width), BF),
            sds((2 * OWN, width), BF),
            sds((N_DP, TGT, 2 * WIDE), BF),
            sds((OWN, LANES), F32),
        ),
        scratch=(
            pltpu.VMEM((BLOCK, N_Z * LANES), BF),
            pltpu.VMEM((TGT, 2 * WIDE), F32),
            pltpu.VMEM((TGT, N_Z * HEAD_DIM), F32),
            pltpu.VMEM((2 * TGT, width), F32),
            pltpu.VMEM((TGT, LANES), F32),
        ),
        in_specs=[SMEM, SMEM] + [pl.BlockSpec()] * 5,
    )(grp_at, core_at, on_chip(mixed), perm, target_out, out_mine, on_chip(out_other))
    got = lax.ppermute(send, "grp", SWAP)
    mixed_all = exchange(mixed_c, DP)
    mixed_all = mixed_all.reshape(N_DP * TGT, 2 * WIDE)
    stripes = call(
        slope_kernel, sds((2 * N_DP, OWN, 256), BF), scratch=(pltpu.VMEM((OWN, width), F32),)
    )(keep, on_chip(got), tokens_own, seeds, count)
    stripes = after(stripes, mixed_all)
    arrived = lax.all_to_all(stripes, (*DP, "grp"), split_axis=0, concat_axis=0, tiled=True)
    grad = lax.dot_general(
        arrived.reshape(N_DP * TGT, 256),
        mixed_all,
        (((0,), (0,)), ((), ())),
        preferred_element_type=F32,
    )
    lower, upper = (grad[: 16 * N_Z], grad[16 * N_Z :])
    grad_keep = jnp.where(core == 0, lower, upper)
    grad_send = jnp.where(core == 0, upper, lower)
    grad = grad_keep + lax.ppermute(grad_send, "core", SWAP)
    grad = grad.astype(BF).reshape(N_Z, 16, 2 * WIDE)
    pieces = exchange(grad, "z")
    turned = pl.BlockSpec((LANES, WIDE), lambda i: (i, 0))
    target_blend = call(
        blend_kernel,
        sds((half, width), F32),
        grid=(width // LANES,),
        in_specs=[SMEM, pl.BlockSpec((half, LANES), lambda i: (0, i)), turned, turned],
        out_specs=pl.BlockSpec((half, LANES), lambda i: (0, i)),
    )(core_at, after(target_out, grad), out_mine, out_other)
    grad = jnp.sum(pieces.astype(F32), axis=0).astype(BF)
    grad = to_all(after(grad, target_blend), "z", N_Z).reshape(16 * N_Z, 2 * WIDE)
    other = lax.ppermute(grad, "core", SWAP)
    out_grad = call(
        finish_kernel,
        sds((student_out.shape[1], student_out.shape[0]), F32),
        in_specs=[SMEM] + [pl.BlockSpec()] * 2,
    )(core_at, on_chip(grad), on_chip(other)).T
    return (out_grad, target_blend)


def solution(mesh):
    fine = Mesh(mesh.devices.reshape(8, 2, 2, 2, 4), ("z", "core", "grp", "ylo", "x"))
    seq = ("z", "core")
    in_specs = (
        P(DP, seq, None),
        P(DP, seq),
        P(DP, seq),
        P(None, DP, "grp"),
        P("grp", None),
        P(None, DP, "grp"),
        P("grp", DP),
        P(),
    )
    out_specs = (P("grp", DP), P("grp", None))
    return jax.shard_map(body, mesh=fine, in_specs=in_specs, out_specs=out_specs, check_vma=False)
```
